32 devices in a mesh: grp: 8 (over z, x), wide: 4 (over y, core).
Axes of the slice: x: 2, y: 2, z: 4, core: 2. Of those that a mesh axis runs over, the one named last changes fastest.
Arguments:
- velocity: float32 [3, 512, 32, 128], P(None, 'grp', 'wide'), may hold values from -6 to 6
- coarse_ghost: float32 [3, 512, 8, 128], P(None, 'grp', 'wide'), may hold values from -6 to 6
- viscosity: float32 [512, 32, 128], P('grp', 'wide'), may hold values from 0.5 to 4
- stress: float32 [6, 512, 32, 128], P(None, 'grp', 'wide'), may hold values from -6 to 6
- patch_mask: int32 [8, 8], P('grp', 'wide'), may hold values 0 or 1
- coarse_owner: int32 [8, 8], P('grp', 'wide'), may hold values from 0 to 63, as said below
Outputs:
- new_velocity: float32 [3, 512, 32, 128], P(None, 'grp', 'wide')
- coarse_patch_update: float32 [8, 64, 3, 6144], P('grp', 'wide')
The draws below stay inside these ranges and needn't reach their ends.
Inputs may be any that keep to these rules, and one draw needn't show every extreme that they name: `coarse_owner`: coarse patch c belongs to wide index c // 16. Of the 2 fine patches of one device at most 1 have coarse patches on any one wide index, and in every draw every device sends exactly 1 to one common wide index.
All inputs are finite; a program needn't handle non-finite values. No bound on the sum of `patch_mask` on one device may be relied on, other than what follows from the above.
Results may differ from the reference program's by a relative error of at most 0.000096.
Values sent between devices are 32-bit elements; how exact they have to be, the bound alone decides.
No kernel may reach another device: no remote copies, remote signals or barrier semaphores. Data moves between devices by JAX's collectives and lax.ppermute only.
A program may use at most 128 MiB of HBM per device.

```python
import math
import jax
import jax.numpy as jnp
from jax import lax

PATCH = 64
CY = 8
P_SIZE = 2
CP_DEV = 16
SWEEPS = 3
CAP = 1
CZ = 128
NX = 512
NY = 32
PV = 6144
CPW = 64
N_GRP = 8
N_WIDE = 4


def draw_coarse_owner(key, part):
    slot_count = N_WIDE * CAP
    favoured = jax.random.randint(jax.random.fold_in(key, 11), (), 0, N_WIDE)

    def one_device(device_index):
        dev_key = jax.random.fold_in(key, 100 + device_index)
        ranks = jax.random.permutation(jax.random.fold_in(dev_key, 1), slot_count)
        slot_ids = jnp.arange(slot_count)
        scores = jnp.where(slot_ids // CAP == favoured, slot_ids - slot_count, ranks)
        chosen = jnp.argsort(scores, stable=True)[:P_SIZE]
        chosen = jax.random.permutation(jax.random.fold_in(dev_key, 2), chosen)
        local_ids = jax.random.randint(jax.random.fold_in(dev_key, 3), (P_SIZE,), 0, CP_DEV)
        return chosen // CAP * CP_DEV + local_ids
    table = jax.vmap(one_device)(jnp.arange(N_GRP * N_WIDE))
    return table.reshape(N_GRP, N_WIDE * P_SIZE).astype(jnp.int32)


def plant(values, own_key, smallest, top_value):
    index_at = [jax.random.randint(jax.random.fold_in(own_key, axis), (), 0, length) for axis, length in enumerate(values.shape)]
    main_axis = values.shape.index(max(values.shape))
    next_to = index_at[:main_axis] + [(index_at[main_axis] + 1) % values.shape[main_axis]] + index_at[main_axis + 1:]
    return values.at[tuple(index_at)].set(smallest).at[tuple(next_to)].set(top_value)


def block_scale(key, extent, shards, least, top_value):
    level, own = 1.0, jax.random.fold_in(key, 6)
    for axis_at, parts in shards:
        steps = jnp.exp(jax.random.uniform(jax.random.fold_in(own, axis_at), (parts,), jnp.float32, least / len(shards), top_value / len(shards)))
        level = level * jnp.repeat(steps, extent[axis_at] // parts).reshape([-1 if axis == axis_at else 1 for axis in range(len(extent))])
    return level


def scatter_about(stream_key, extent, scale, most, pieces=(), kind=jnp.bfloat16):
    entries = scale * jax.random.normal(stream_key, extent, jnp.float32)
    if pieces:
        entries = entries * block_scale(stream_key, extent, pieces, -0.22, 0.18)
    return jnp.clip(entries, -most, most).astype(kind)


def setup_inputs(seed: int = 0) -> dict:
    key_of = jax.random.split(jax.random.key(seed), 7)
    return {
        "velocity": scatter_about(key_of[0], (3, NX, NY, CZ), 1.0, 6.0, ((1, 8), (2, 4)), jnp.float32),
        "coarse_ghost": scatter_about(key_of[1], (3, NX, 2 * N_WIDE, CZ), 1.0, 6.0, ((1, 8), (2, 4)), jnp.float32),
        "viscosity": jnp.clip(jnp.exp(math.log(4.0) - 2.0794415 * jax.random.uniform(key_of[2], (NX, NY, CZ), jnp.float32) ** block_scale(key_of[2], (NX, NY, CZ), ((0, 8), (1, 4)), -0.2, 0.2)), 0.5, 4.0),
        "stress": scatter_about(key_of[3], (6, NX, NY, CZ), 1.0, 6.0, ((1, 8), (2, 4)), jnp.float32),
        "patch_mask": plant((jax.random.randint(key_of[4], (N_GRP, N_WIDE * P_SIZE), 0, 4) < 3).astype(jnp.int32), jax.random.fold_in(key_of[4], 1), 0, 1),
        "coarse_owner": draw_coarse_owner(jax.random.fold_in(key_of[6], 71), 0),
    }


KAPPA = 1.0
OMEGA = 0.8


def apply_operator(values_in, visc_pad):
    centre_cell = visc_pad[1:-1, 1:-1]
    visc_east = 0.5 * (centre_cell + visc_pad[2:, 1:-1])
    visc_west = 0.5 * (centre_cell + visc_pad[:-2, 1:-1])
    visc_north = 0.5 * (centre_cell + visc_pad[1:-1, 2:])
    visc_south = 0.5 * (centre_cell + visc_pad[1:-1, :-2])
    visc_up = 0.5 * (centre_cell + jnp.roll(centre_cell, -1, axis=2))
    visc_down = 0.5 * (centre_cell + jnp.roll(centre_cell, 1, axis=2))
    interior = values_in[:, 1:-1, 1:-1]
    diffusion = visc_east * (values_in[:, 2:, 1:-1] - interior) - visc_west * (interior - values_in[:, :-2, 1:-1])
    diffusion = diffusion + visc_north * (values_in[:, 1:-1, 2:] - interior) - visc_south * (interior - values_in[:, 1:-1, :-2])
    diffusion = diffusion + visc_up * (jnp.roll(interior, -1, axis=3) - interior) - visc_down * (interior - jnp.roll(interior, 1, axis=3))
    diagonal = KAPPA + visc_east + visc_west + visc_north + visc_south + visc_up + visc_down
    return KAPPA * interior - diffusion, diagonal


def divergence(stress_pad):
    def diff_x(comp):
        return 0.5 * (comp[2:, 1:-1] - comp[:-2, 1:-1])

    def diff_y(comp):
        return 0.5 * (comp[1:-1, 2:] - comp[1:-1, :-2])

    def diff_z(comp):
        middle = comp[1:-1, 1:-1]
        return 0.5 * (jnp.roll(middle, -1, axis=2) - jnp.roll(middle, 1, axis=2))

    force_x = diff_x(stress_pad[0]) + diff_y(stress_pad[3]) + diff_z(stress_pad[4])
    force_y = diff_x(stress_pad[3]) + diff_y(stress_pad[1]) + diff_z(stress_pad[5])
    force_z = diff_x(stress_pad[4]) + diff_y(stress_pad[5]) + diff_z(stress_pad[2])
    return jnp.stack([force_x, force_y, force_z], axis=0)


def patch_data(residual, smoothed, viscosity, coarse_ghost, groups):
    half = PATCH // 2
    blocks = residual.reshape(3, groups, half, 2, CY // 2, 2, P_SIZE, half, 2).mean(axis=(3, 5, 8))
    blocks = jnp.transpose(blocks, (1, 4, 0, 2, 3, 5)).reshape(groups, P_SIZE, 3, half * (CY // 2) * half)
    flux_low = viscosity[:, 0, :] * (smoothed[:, :, 0, :] - coarse_ghost[:, :, 0, :])
    flux_high = viscosity[:, -1, :] * (coarse_ghost[:, :, 1, :] - smoothed[:, :, -1, :])

    def faces(flux):
        reduced_terms = flux.reshape(3, groups, half, 2, P_SIZE, half, 2).mean(axis=(3, 6))
        return jnp.transpose(reduced_terms, (1, 3, 0, 2, 4)).reshape(groups, P_SIZE, 3, half * half)

    return jnp.concatenate([blocks, faces(flux_low), faces(flux_high)], axis=3)


def column(velocity, coarse_ghost, viscosity, stress):
    vel_field = jnp.concatenate([coarse_ghost[:, :, :1], velocity, coarse_ghost[:, :, 1:]], axis=2)
    vel_field = jnp.pad(vel_field, ((0, 0), (1, 1), (0, 0), (0, 0)))
    visc_pad = jnp.concatenate([viscosity[:, :1], viscosity, viscosity[:, -1:]], axis=1)
    visc_pad = jnp.pad(visc_pad, ((1, 1), (0, 0), (0, 0)))
    stress_pad = jnp.pad(stress, ((0, 0), (1, 1), (1, 1), (0, 0)))
    source = KAPPA * velocity + divergence(stress_pad)
    for sweep_index in range(SWEEPS):
        applied, diagonal = apply_operator(vel_field, visc_pad)
        interior = vel_field[:, 1:-1, 1:-1]
        updated = interior + OMEGA * (source - applied) / diagonal
        vel_field = vel_field.at[:, 1:-1, 1:-1].set(updated)
    applied, diagonal = apply_operator(vel_field, visc_pad)
    residual = source - applied
    smoothed = vel_field[:, 1:-1, 1:-1]
    return smoothed, patch_data(residual, smoothed, viscosity, coarse_ghost, N_GRP)


def reference(velocity, coarse_ghost, viscosity, stress, patch_mask, coarse_owner):
    vel_cols = jnp.moveaxis(velocity.reshape(3, NX, N_WIDE, CY, CZ), 2, 0)
    ghost_cols = jnp.moveaxis(coarse_ghost.reshape(3, NX, N_WIDE, 2, CZ), 2, 0)
    visc_cols = jnp.moveaxis(viscosity.reshape(NX, N_WIDE, CY, CZ), 1, 0)
    stress_cols = jnp.moveaxis(stress.reshape(6, NX, N_WIDE, CY, CZ), 2, 0)
    smoothed, fine_patches = lax.map(lambda items: column(*items), (vel_cols, ghost_cols, visc_cols, stress_cols))
    new_velocity = jnp.moveaxis(smoothed, 0, 2).reshape(3, NX, NY, CZ)
    fine_patches = jnp.transpose(fine_patches, (1, 0, 2, 3, 4)).reshape(N_GRP, N_WIDE * P_SIZE, 3 * PV)
    fine_patches = fine_patches * patch_mask[:, :, None].astype(jnp.float32)
    indicator_matrix = (coarse_owner[:, None, :] == jnp.arange(CPW, dtype=jnp.int32)[None, :, None]).astype(jnp.float32)
    coarse_patch_update = jnp.einsum("xjn,xnd->xjd", indicator_matrix, fine_patches, precision=lax.Precision.HIGHEST)
    return new_velocity, coarse_patch_update.reshape(N_GRP, CPW, 3, PV)
```

```python
import functools

import jax
import jax.numpy as jnp
import numpy as np
from jax import lax
from jax.experimental import pallas as pl
from jax.experimental.pallas import tpu as pltpu
from jax.sharding import PartitionSpec as P

PATCH = 64
CY = 8
P_SIZE = 2
CP_DEV = 16
SWEEPS = 3
PV = 6144

KAPPA = 1.0
OMEGA = 0.8

R_U = 0
R_V = 96
R_F = 128
R_S = 200
R_G = 224
PACK = 248

T_U = 0
T_C = 18
T_G = 39
STATE = 48

HALF = PATCH // 2
ROWS_C = HALF + 2 * (HALF // 4)
SLOT = 3 * ROWS_C + 8
UNROLL = 10


def pool_matrix(cz):
    k = np.arange(4 * cz)[:, None]
    n = np.arange(P_SIZE * cz)[None, :]
    same_row = (k // cz) == (n % cz) // HALF
    same_col = (k % cz) // 2 == (n // cz) * HALF + n % HALF
    return (same_row & same_col).astype(np.float32)


def up_z(v):
    return pltpu.roll(v, v.shape[1] - 1, 1)


def down_z(v):
    return pltpu.roll(v, 1, 1)


def north_of(v, high):
    row = lax.broadcasted_iota(jnp.int32, v.shape, 0)
    return jnp.where(row == CY - 1, high, pltpu.roll(v, CY - 1, 0))


def south_of(v, low):
    row = lax.broadcasted_iota(jnp.int32, v.shape, 0)
    return jnp.where(row == 0, low, pltpu.roll(v, 1, 0))


def edge_rows(v):
    row = lax.broadcasted_iota(jnp.int32, v.shape, 0)
    north = jnp.where(row == CY - 1, v, pltpu.roll(v, CY - 1, 0))
    south = jnp.where(row == 0, v, pltpu.roll(v, 1, 0))
    return north, south


def diff_y(v):
    row = lax.broadcasted_iota(jnp.int32, v.shape, 0)
    north = jnp.where(row == CY - 1, 0.0, pltpu.roll(v, CY - 1, 0))
    south = jnp.where(row == 0, 0.0, pltpu.roll(v, 1, 0))
    return north - south


def diff_z(v):
    return up_z(v) - down_z(v)


def coefficients(v, v_west, v_east):
    v_north, v_south = edge_rows(v)
    half = 0.5 * v
    east = half + 0.5 * v_east
    west = half + 0.5 * v_west
    north = half + 0.5 * v_north
    south = half + 0.5 * v_south
    up = half + 0.5 * up_z(v)
    down = down_z(up)
    diagonal = KAPPA + ((east + west) + (north + south)) + (up + down)
    scale = OMEGA / diagonal
    return (
        [scale * west, scale * east, scale * south, scale * north, scale * down, scale * up],
        diagonal * (1.0 / OMEGA),
        scale,
    )


def gather_terms(g, c, u, u_west, u_east, low, high):
    x = c[0] * u_west + c[1] * u_east
    y = c[2] * south_of(u, low) + c[3] * north_of(u, high)
    z = c[4] * down_z(u) + c[5] * up_z(u)
    return (g + x) + (y + z)


def pack_kernel(vel, ghost, visc, stress, out_a, out_b, u_s, v_s, s_s, g_s, sem):
    rows = vel.shape[1]
    copies = []
    for side in range(2):
        r0 = 0 if side == 0 else rows - 4 * CY
        g0 = 0 if side == 0 else ghost.shape[1] - 8
        for n, (src, dst) in enumerate(
            (
                (stress.at[:, pl.ds(r0, 4 * CY)], s_s.at[side]),
                (vel.at[:, pl.ds(r0, 4 * CY)], u_s.at[side]),
                (visc.at[pl.ds(r0, 4 * CY)], v_s.at[side]),
                (ghost.at[:, pl.ds(g0, 8)], g_s.at[side]),
            )
        ):
            copies.append(pltpu.make_async_copy(src, dst, sem.at[side, n]))
    for c in copies:
        c.start()
    for c in copies:
        c.wait()
    even = lax.axis_index("grp") % 2 == 0

    def plane(ref, side, comp, p):
        return ref[side, comp, p * CY : (p + 1) * CY, :]

    packs = []
    for side in range(2):
        parts = {}
        for c in range(3):
            parts[R_U + c * 32] = u_s[side, c]
        parts[R_V] = v_s[side]
        for j in range(3):
            p = j if side == 0 else j + 1

            def dx(comp):
                if p == 0:
                    return plane(s_s, side, comp, p + 1)
                if p == 3:
                    return -plane(s_s, side, comp, p - 1)
                return plane(s_s, side, comp, p + 1) - plane(s_s, side, comp, p - 1)

            xx, yy, zz, xy, xz, yz = range(6)
            s_xy, s_xz, s_yz = (plane(s_s, side, k, p) for k in (xy, xz, yz))
            s_yy, s_zz = (plane(s_s, side, k, p) for k in (yy, zz))
            f = (
                dx(xx) + diff_y(s_xy) + diff_z(s_xz),
                dx(xy) + diff_y(s_yy) + diff_z(s_yz),
                dx(xz) + diff_y(s_yz) + diff_z(s_zz),
            )
            for c in range(3):
                parts[R_F + (c * 3 + j) * CY] = KAPPA * plane(u_s, side, c, p) + 0.5 * f[c]
        edge = 0 if side == 0 else 3
        for c, k in enumerate((xx, xy, xz)):
            parts[R_S + c * CY] = plane(s_s, side, k, edge)
        for c in range(3):
            parts[R_G + c * 8] = g_s[side, c]
        packs.append(parts)
    for r, low in packs[0].items():
        high = packs[1][r]
        out_a[r : r + low.shape[0], :] = jnp.where(even, high, low)
        out_b[r : r + low.shape[0], :] = jnp.where(even, low, high)


def split_dot(x, m):
    hi = x.astype(jnp.bfloat16)
    rest = x - hi.astype(jnp.float32)
    mid = rest.astype(jnp.bfloat16)
    lo = (rest - mid.astype(jnp.float32)).astype(jnp.bfloat16)
    dot = functools.partial(jnp.dot, preferred_element_type=jnp.float32)
    return dot(hi, m) + (dot(mid, m) + dot(lo, m))


def over_planes(first, last, unroll, body):
    steps = (last - first) // unroll

    def step(t, _):
        for j in range(unroll):
            body(first + t * unroll + j)
        return 0

    lax.fori_loop(0, steps, step, 0)
    for i in range(first + steps * unroll, last):
        body(i)


def interior_kernel(
    vel, ghost, visc, stress, pool, new_v, state, pooled, coef, gsrc, ua, ub, s_sum, flux, xmat
):
    planes = visc.shape[0] // CY
    cz = visc.shape[1]

    def at(i):
        return pl.ds(i * CY if isinstance(i, int) else pl.multiple_of(i * CY, CY), CY)

    def ghosts(c, i):
        return ghost[c, pl.ds(2 * i, 1), :], ghost[c, pl.ds(2 * i + 1, 1), :]

    def first(i):
        c, diag, scale = coefficients(visc[at(i)], visc[at(i - 1)], visc[at(i + 1)])
        for k in range(6):
            coef[k, at(i)] = c[k]
        coef[6, at(i)] = diag

        def dx(k):
            return stress[k, at(i + 1)] - stress[k, at(i - 1)]

        s_xy, s_xz, s_yz = (stress[k, at(i)] for k in (3, 4, 5))
        f = (
            dx(0) + diff_y(s_xy) + diff_z(s_xz),
            dx(3) + diff_y(stress[1, at(i)]) + diff_z(s_yz),
            dx(4) + diff_y(s_yz) + diff_z(stress[2, at(i)]),
        )
        for k in range(3):
            u = vel[k, at(i)]
            g = scale * (KAPPA * u + 0.5 * f[k])
            gsrc[k, at(i)] = g
            low, high = ghosts(k, i)
            t = gather_terms(g, c, u, vel[k, at(i - 1)], vel[k, at(i + 1)], low, high)
            ua[k, at(i)] = (1.0 - OMEGA) * u + t

    over_planes(1, planes - 1, UNROLL, first)

    def sweep(src, dst):
        def body(i):
            c = [coef[k, at(i)] for k in range(6)]
            for k in range(3):
                u = src[k, at(i)]
                low, high = ghosts(k, i)
                t = gather_terms(
                    gsrc[k, at(i)], c, u, src[k, at(i - 1)], src[k, at(i + 1)], low, high
                )
                dst[k, at(i)] = (1.0 - OMEGA) * u + t

        return body

    over_planes(2, planes - 2, UNROLL, sweep(ua, ub))
    over_planes(3, planes - 3, UNROLL, sweep(ub, new_v))

    s_sum[...] = jnp.zeros_like(s_sum)

    def residuals(b):
        for k in range(3):
            total = None
            for j in range(2):
                i = 2 * b + j
                c = [coef[n, at(i)] for n in range(6)]
                u = new_v[k, at(i)]
                low, high = ghosts(k, i)
                t = gather_terms(
                    gsrc[k, at(i)], c, u, new_v[k, at(i - 1)], new_v[k, at(i + 1)], low, high
                )
                r = (t - OMEGA * u) * coef[6, at(i)]
                total = r if total is None else total + r
            s_sum[k, at(b)] = total

    over_planes(2, planes // 2 - 2, UNROLL // 2, residuals)

    keep = lax.broadcasted_iota(jnp.int32, (planes, cz), 0)
    keep = (keep >= SWEEPS) & (keep < planes - SWEEPS)
    for k in range(3):
        for face in range(2):
            row = 0 if face == 0 else CY - 1
            nu = visc[pl.ds(row, planes, stride=CY), :]
            cell = new_v[k, pl.ds(row, planes, stride=CY), :]
            outer = ghost[k, pl.ds(face, planes, stride=2), :]
            value = nu * (cell - outer) if face == 0 else nu * (outer - cell)
            flux[...] = jnp.where(keep, value, 0.0)
            for j in range(4):
                both = flux[pl.ds(2 * j, planes // 8, stride=8), :] + flux[
                    pl.ds(2 * j + 1, planes // 8, stride=8), :
                ]
                base = k * ROWS_C + HALF + face * (HALF // 4)
                xmat[base : base + HALF // 4, j * cz : (j + 1) * cz] = 0.25 * both
        for j in range(4):
            both = s_sum[k, pl.ds(2 * j, planes // 2, stride=CY), :] + s_sum[
                k, pl.ds(2 * j + 1, planes // 2, stride=CY), :
            ]
            xmat[k * ROWS_C : k * ROWS_C + HALF, j * cz : (j + 1) * cz] = 0.125 * both
    pooled[...] = split_dot(xmat[...], pool[...])

    for side in range(2):

        def depth(d):
            i = d if side == 0 else planes - 1 - d
            return slice(i * CY, (i + 1) * CY)

        def put(n, value):
            state[side, n * CY : (n + 1) * CY, :] = value

        for s, ref in ((1, ua), (2, ub), (3, new_v)):
            for k in range(3):
                for e in range(2):
                    put(T_U + (s - 1) * 6 + k * 2 + e, ref[k, depth(s + e), :])
        for d in range(1, 4):
            for n in range(7):
                put(T_C + n * 3 + d - 1, coef[n, depth(d), :])
            for k in range(3):
                put(T_G + k * 3 + d - 1, gsrc[k, depth(d), :])


def edge_kernel(
    n_wide,
    owner,
    mask,
    in_a,
    in_b,
    got_a,
    got_b,
    state,
    pooled,
    pool,
    velocity_in,
    velocity_out,
    *refs,
):
    slots = refs[:n_wide]
    u_out, xmat, flux, total_s, out_sem = refs[n_wide:]
    del velocity_in
    grp = lax.axis_index("grp")
    even = grp % 2 == 0
    ends = (grp > 0, grp < lax.axis_size("grp") - 1)

    cz = pool.shape[0] // 4
    xmat[...] = jnp.zeros_like(xmat)
    flux[...] = jnp.zeros_like(flux)
    for side in range(2):
        sign = -1.0 if side == 0 else 1.0
        inside = jnp.where(ends[side], 1.0, 0.0)

        def index(q, count):
            if q >= 0:
                return q if side == 0 else count - 1 - q
            return count + q if side == 0 else -q - 1

        def get(q, start, comp, count, rows=CY):
            r = start + (comp * count + index(q, count)) * rows
            return packed(q >= 0, r, rows)

        def packed(own, r, rows=CY):
            a, b = (in_a, in_b) if own else (got_a, got_b)
            a, b = a[r : r + rows, :], b[r : r + rows, :]
            return jnp.where(even, b, a) if side == 0 else jnp.where(even, a, b)

        def saved(n):
            return state[side, n * CY : (n + 1) * CY, :]

        visc = {q: get(q, R_V, 0, 4) for q in range(-4, 2)}
        ghost = {
            (k, q): get(q, R_G, k, 4, 2) for k in range(3) for q in range(-3, 4)
        }
        coef, diag, g = {}, {}, {}
        for q in range(-3, 1):
            c, d, scale = coefficients(visc[q], visc[q - 1], visc[q + 1])
            coef[q], diag[q] = c, d
            for k in range(3):
                f = get(q, R_F, k, 3)
                if q == 0:
                    f = f + (0.5 * sign) * packed(False, R_S + k * CY)
                if q == -1:
                    f = f - (0.5 * sign) * packed(True, R_S + k * CY)
                g[k, q] = scale * f
        for q in range(1, 4):
            c = [saved(T_C + n * 3 + q - 1) for n in range(7)]
            coef[q], diag[q] = ([c[0], c[1]] if side == 0 else [c[1], c[0]]) + c[2:6], c[6]
            for k in range(3):
                g[k, q] = saved(T_G + k * 3 + q - 1)
        for k in range(3):
            u = {q: get(q, R_U, k, 4) for q in range(-4, 2)}
            for s in range(1, SWEEPS + 1):
                new = {}
                for q in range(s - 4, s):
                    low, high = ghost[k, q][0:1], ghost[k, q][1:2]
                    t = gather_terms(g[k, q], coef[q], u[q], u[q - 1], u[q + 1], low, high)
                    value = (1.0 - OMEGA) * u[q] + t
                    new[q] = value * inside if q < 0 else value
                for e in range(2):
                    new[s + e] = saved(T_U + (s - 1) * 6 + k * 2 + e)
                u = new
            for q in range(3):
                i = q if side == 0 else 2 - q
                u_out[side, k, i * CY : (i + 1) * CY, :] = u[q]
            sums = []
            for b in range(2):
                total = None
                for q in (2 * b, 2 * b + 1):
                    low, high = ghost[k, q][0:1], ghost[k, q][1:2]
                    t = gather_terms(g[k, q], coef[q], u[q], u[q - 1], u[q + 1], low, high)
                    r = (t - OMEGA * u[q]) * diag[q]
                    total = r if total is None else total + r
                sums.append(total)
            for b in range(2):
                row = b if side == 0 else 3 - b
                both = sums[b] + pltpu.roll(sums[b], CY - 1, 0)
                for j in range(4):
                    xmat[k * 8 + row : k * 8 + row + 1, j * cz : (j + 1) * cz] = (
                        0.125 * both[2 * j : 2 * j + 1, :]
                    )
            for q in range(3):
                x = q if side == 0 else 7 - q
                nu = get(q, R_V, 0, 4)
                low, high = ghost[k, q][0:1], ghost[k, q][1:2]
                flux[side, k, 0, x : x + 1, :] = nu[0:1] * (u[q][0:1] - low)
                flux[side, k, 1, x : x + 1, :] = nu[CY - 1 :] * (high - u[q][CY - 1 :])
            for face in range(2):
                for j in range(4):
                    row = k * 8 + 4 + face * 2 + side
                    xmat[row : row + 1, j * cz : (j + 1) * cz] = 0.25 * (
                        flux[side, k, face, 2 * j : 2 * j + 1, :]
                        + flux[side, k, face, 2 * j + 1 : 2 * j + 2, :]
                    )
    rows = velocity_out.shape[1]
    out_copies = [
        pltpu.make_async_copy(
            u_out.at[side],
            velocity_out.at[:, pl.ds(0 if side == 0 else rows - 3 * CY, 3 * CY)],
            out_sem.at[side],
        )
        for side in range(2)
    ]
    for c in out_copies:
        c.start()

    edge = split_dot(xmat[...], pool[...])
    places = (0, 1, HALF - 2, HALF - 1, HALF, HALF + HALF // 4 - 1, HALF + HALF // 4, ROWS_C - 1)
    total_s[...] = pooled[...]
    for k in range(3):
        for n, place in enumerate(places):
            r = k * ROWS_C + place
            total_s[r : r + 1, :] = total_s[r : r + 1, :] + edge[k * 8 + n : k * 8 + n + 1, :]
    me = lax.axis_index("wide")
    for d in range(n_wide):
        value, local = None, jnp.float32(-1.0)
        for p in range(P_SIZE):
            match = owner[0, p] // CP_DEV == me ^ d
            weight = jnp.where(match, mask[0, p], 0).astype(jnp.float32)
            local = jnp.where(match, (owner[0, p] % CP_DEV).astype(jnp.float32), local)
            term = total_s[:, p * cz : (p + 1) * cz] * weight
            value = term if value is None else value + term
        slots[d][0 : 3 * ROWS_C, :] = value
        slots[d][3 * ROWS_C :, :] = jnp.full((8, cz), local, jnp.float32)
    for c in out_copies:
        c.wait()


def collect_kernel(n_wide, *refs):
    slots, out = refs[:n_wide], refs[n_wide]
    cz = slots[0].shape[1]
    rows = lax.broadcasted_iota(jnp.int32, (CP_DEV, cz), 0).astype(jnp.float32)
    takes = [rows == slot[3 * ROWS_C : 3 * ROWS_C + 1, :] for slot in slots]
    for k in range(3):
        for n in range(ROWS_C):
            total = None
            for take, slot in zip(takes, slots, strict=True):
                r = k * ROWS_C + n
                term = jnp.where(take, slot[r : r + 1, :], 0.0)
                total = term if total is None else total + term
            out[k, :, n * cz : (n + 1) * cz] = total


def on_device(velocity, coarse_ghost, viscosity, stress, patch_mask, coarse_owner):
    n_grp, n_wide = lax.axis_size("grp"), lax.axis_size("wide")
    cells_x, cz = viscosity.shape[0], viscosity.shape[2]
    f32 = jnp.float32
    vel = velocity.reshape(3, cells_x * CY, cz)
    ghost = coarse_ghost.reshape(3, cells_x * 2, cz)
    visc = viscosity.reshape(cells_x * CY, cz)
    strs = stress.reshape(6, cells_x * CY, cz)
    pool = jnp.asarray(pool_matrix(cz), jnp.bfloat16)

    anywhere = pl.BlockSpec(memory_space=pl.ANY)
    vmem = pl.BlockSpec(memory_space=pltpu.VMEM)
    smem = pl.BlockSpec(memory_space=pltpu.SMEM)
    pack_shape = jax.ShapeDtypeStruct((PACK, cz), f32)
    pack_a, pack_b = pl.pallas_call(
        pack_kernel,
        out_shape=(pack_shape, pack_shape),
        in_specs=[anywhere] * 4,
        out_specs=(vmem, vmem),
        scratch_shapes=[
            pltpu.VMEM((2, 3, 4 * CY, cz), f32),
            pltpu.VMEM((2, 4 * CY, cz), f32),
            pltpu.VMEM((2, 6, 4 * CY, cz), f32),
            pltpu.VMEM((2, 3, 8, cz), f32),
            pltpu.SemaphoreType.DMA((2, 4)),
        ],
        name="pack",
    )(vel, ghost, visc, strs)

    pairs_a = [(i, i ^ 1) for i in range(n_grp) if i ^ 1 < n_grp]
    pairs_b = [(i, j) for i in range(n_grp) for j in [((i + 1) ^ 1) - 1] if 0 <= j < n_grp]
    got_b = lax.ppermute(pack_b, "grp", pairs_b)
    got_a = lax.ppermute(pack_a, "grp", pairs_a)

    rows = cells_x * CY
    new_v, state, pooled = pl.pallas_call(
        interior_kernel,
        out_shape=(
            jax.ShapeDtypeStruct((3, rows, cz), f32),
            jax.ShapeDtypeStruct((2, STATE * CY, cz), f32),
            jax.ShapeDtypeStruct((3 * ROWS_C, P_SIZE * cz), f32),
        ),
        in_specs=[vmem] * 5,
        out_specs=(vmem, vmem, vmem),
        scratch_shapes=[
            pltpu.VMEM((7, rows, cz), f32),
            pltpu.VMEM((3, rows, cz), f32),
            pltpu.VMEM((3, rows, cz), f32),
            pltpu.VMEM((3, rows, cz), f32),
            pltpu.VMEM((3, rows // 2, cz), f32),
            pltpu.VMEM((cells_x, cz), f32),
            pltpu.VMEM((3 * ROWS_C, 4 * cz), f32),
        ],
        cost_estimate=pl.CostEstimate(flops=100_000_000, bytes_accessed=4_000_000, transcendentals=0),
        name="interior",
    )(vel, ghost, visc, strs, pool)

    slot_shape = jax.ShapeDtypeStruct((SLOT, cz), f32)
    outs = pl.pallas_call(
        functools.partial(edge_kernel, n_wide),
        out_shape=(jax.ShapeDtypeStruct(new_v.shape, f32),) + (slot_shape,) * n_wide,
        in_specs=[smem, smem] + [vmem] * 7 + [anywhere],
        out_specs=(anywhere,) + (vmem,) * n_wide,
        scratch_shapes=[
            pltpu.VMEM((2, 3, 3 * CY, cz), f32),
            pltpu.VMEM((24, 4 * cz), f32),
            pltpu.VMEM((2, 3, 2, 8, cz), f32),
            pltpu.VMEM((3 * ROWS_C, P_SIZE * cz), f32),
            pltpu.SemaphoreType.DMA((2,)),
        ],
        input_output_aliases={9: 0},
        name="edge",
    )(coarse_owner, patch_mask, pack_a, pack_b, got_a, got_b, state, pooled, pool, new_v)
    smoothed, slots = outs[0], list(outs[1:])

    for k in range(1, n_wide):
        slots[k] = lax.ppermute(slots[k], "wide", [(i, i ^ k) for i in range(n_wide)])
    coarse = pl.pallas_call(
        functools.partial(collect_kernel, n_wide),
        out_shape=jax.ShapeDtypeStruct((3, CP_DEV, PV), f32),
        in_specs=[vmem] * n_wide,
        out_specs=vmem,
        name="collect",
    )(*slots)
    return smoothed.reshape(velocity.shape), coarse.transpose(1, 0, 2)[None]


def solution(mesh):
    in_specs = (
        P(None, "grp", "wide", None),
        P(None, "grp", "wide", None),
        P("grp", "wide", None),
        P(None, "grp", "wide", None),
        P("grp", "wide"),
        P("grp", "wide"),
    )
    out_specs = (P(None, "grp", "wide", None), P("grp", "wide", None, None))
    return jax.shard_map(
        on_device, mesh=mesh, in_specs=in_specs, out_specs=out_specs, check_vma=False
    )
```

```python
import functools

import jax
import jax.numpy as jnp
import numpy as np
from jax import lax
from jax.experimental import pallas as pl
from jax.experimental.pallas import tpu as pltpu
from jax.sharding import PartitionSpec as P

PATCH = 64
CY = 8
P_SIZE = 2
CP_DEV = 16
SWEEPS = 3
PV = 6144

KAPPA = 1.0
OMEGA = 0.8

R_U = 0
R_P = 24
R_S = 96
R_V = 120
R_N = 128
R_E = 136
R_G = 144
PACK = 152

T_U = 0
T_C = 18
T_G = 39
STATE = 48

HALF = PATCH // 2
ROWS_C = HALF + 2 * (HALF // 4)
SLOT = 3 * ROWS_C + 8
UNROLL = 31

MID = HALF // 4 - 2
ROW_ORDER = (
    [0, 1, HALF - 2, HALF - 1, HALF, HALF + MID + 1, HALF + MID + 2, ROWS_C - 1]
    + list(range(2, HALF - 2))
    + list(range(HALF + 1, HALF + MID + 1))
    + list(range(HALF + MID + 3, ROWS_C - 1))
)


def pool_matrix(cz):
    k = np.arange(4 * cz)[:, None]
    n = np.arange(P_SIZE * cz)[None, :]
    same_row = (k // cz) == (n % cz) // HALF
    same_col = (k % cz) // 2 == (n // cz) * HALF + n % HALF
    return (same_row & same_col).astype(np.float32)


def up_z(v):
    return pltpu.roll(v, v.shape[1] - 1, 1)


def down_z(v):
    return pltpu.roll(v, 1, 1)


def north_of(v, high):
    row = lax.broadcasted_iota(jnp.int32, v.shape, 0)
    return jnp.where(row == CY - 1, high, pltpu.roll(v, CY - 1, 0))


def south_of(v, low):
    row = lax.broadcasted_iota(jnp.int32, v.shape, 0)
    return jnp.where(row == 0, low, pltpu.roll(v, 1, 0))


def edge_rows(v):
    row = lax.broadcasted_iota(jnp.int32, v.shape, 0)
    north = jnp.where(row == CY - 1, v, pltpu.roll(v, CY - 1, 0))
    south = jnp.where(row == 0, v, pltpu.roll(v, 1, 0))
    return north, south


def diff_y(v):
    row = lax.broadcasted_iota(jnp.int32, v.shape, 0)
    north = jnp.where(row == CY - 1, 0.0, pltpu.roll(v, CY - 1, 0))
    south = jnp.where(row == 0, 0.0, pltpu.roll(v, 1, 0))
    return north - south


def diff_z(v):
    return up_z(v) - down_z(v)


def coefficients(v, v_west, v_east, west=None):
    v_north, v_south = edge_rows(v)
    half = 0.5 * v
    east = half + 0.5 * v_east
    if west is None:
        west = half + 0.5 * v_west
    north = half + 0.5 * v_north
    south = half + 0.5 * v_south
    up = half + 0.5 * up_z(v)
    down = down_z(up)
    diagonal = KAPPA + ((east + west) + (north + south)) + (up + down)
    scale = OMEGA / diagonal
    return (
        [scale * west, scale * east, scale * south, scale * north, scale * down, scale * up],
        diagonal * (1.0 / OMEGA),
        scale,
    )


def side_terms(c, u, low, high):
    y = c[2] * south_of(u, low) + c[3] * north_of(u, high)
    z = c[4] * down_z(u) + c[5] * up_z(u)
    return y + z


def gather_terms(g, c, u, u_west, u_east, low, high):
    x = c[0] * u_west + c[1] * u_east
    return (g + x) + side_terms(c, u, low, high)


def pack_kernel(vel, ghost, visc, stress, out_a, out_b, own, u_s, v_s, s_s, g_s, sem):
    rows = vel.shape[1]
    copies = []
    for side in range(2):
        r0 = 0 if side == 0 else rows - 4 * CY
        g0 = 0 if side == 0 else ghost.shape[1] - 8
        for n, (src, dst) in enumerate(
            (
                (stress.at[:, pl.ds(r0, 4 * CY)], s_s.at[side]),
                (vel.at[:, pl.ds(r0, 4 * CY)], u_s.at[side]),
                (visc.at[pl.ds(r0, 4 * CY)], v_s.at[side]),
                (ghost.at[:, pl.ds(g0, 8)], g_s.at[side]),
            )
        ):
            copies.append(pltpu.make_async_copy(src, dst, sem.at[side, n]))
    for c in copies:
        c.start()
    for c in copies:
        c.wait()
    even = lax.axis_index("grp") % 2 == 0
    xx, yy, zz, xy, xz, yz = range(6)

    packs = []
    for side in range(2):
        sign = -1.0 if side == 0 else 1.0

        def at(d):
            p = d if side == 0 else 3 - d
            return slice(p * CY, (p + 1) * CY)

        def dx(comp, d):
            inner = s_s[side, comp, at(d + 1), :]
            return -sign * (inner - s_s[side, comp, at(d - 1), :]) if d else -sign * inner

        def ghosts(c, d):
            r = 2 * (d if side == 0 else 3 - d)
            return g_s[side, c, r : r + 1, :], g_s[side, c, r + 1 : r + 2, :]

        force = {}
        for d in range(3):
            s_xy, s_xz, s_yz, s_yy, s_zz = (s_s[side, k, at(d), :] for k in (xy, xz, yz, yy, zz))
            f = (
                dx(xx, d) + diff_y(s_xy) + diff_z(s_xz),
                dx(xy, d) + diff_y(s_yy) + diff_z(s_yz),
                dx(xz, d) + diff_y(s_yz) + diff_z(s_zz),
            )
            for c in range(3):
                force[c, d] = KAPPA * u_s[side, c, at(d), :] + 0.5 * f[c]
        v = [v_s[side, at(d), :] for d in range(4)]
        coef, scale = {}, {}
        for d in (1, 2):
            coef[d], _, scale[d] = coefficients(v[d], v[d - 1], v[d + 1])
        face = 0.5 * v[0] + 0.5 * v[1]
        parts = {R_V: v[0], R_N: face, R_E: face * coef[1][0]}
        for c, k in enumerate((xx, xy, xz)):
            u = [u_s[side, c, at(d), :] for d in range(4)]
            once = {}
            for d in (1, 2):
                low, high = ghosts(c, d)
                t = gather_terms(
                    scale[d] * force[c, d], coef[d], u[d], u[d - 1], u[d + 1], low, high
                )
                once[d] = (1.0 - OMEGA) * u[d] + t
            low, high = ghosts(c, 1)
            rest = side_terms(coef[1], once[1], low, high)
            twice = (1.0 - OMEGA) * once[1] + (
                scale[1] * force[c, 1] + coef[1][1] * once[2] + rest
            )
            for n, inner in enumerate((u[1], once[1], twice)):
                parts[R_P + (n * 3 + c) * CY] = force[c, 0] + face * inner
            parts[R_U + c * CY] = u[0]
            parts[R_S + c * CY] = s_s[side, k, at(0), :]
            own[side, c * CY : (c + 1) * CY, :] = force[c, 0]
            own[side, (3 + c) * CY : (4 + c) * CY, :] = s_s[side, k, at(0), :]
            low, high = ghosts(c, 0)
            parts[R_G + 2 * c], parts[R_G + 2 * c + 1] = low, high
        packs.append(parts)
    for r, low in packs[0].items():
        high = packs[1][r]
        out_a[r : r + low.shape[0], :] = jnp.where(even, high, low)
        out_b[r : r + low.shape[0], :] = jnp.where(even, low, high)
    for out in (out_a, out_b):
        out[R_G + 6 :, :] = jnp.zeros_like(out[R_G + 6 :, :])


def split_dot(x, m):
    hi = x.astype(jnp.bfloat16)
    rest = x - hi.astype(jnp.float32)
    mid = rest.astype(jnp.bfloat16)
    lo = (rest - mid.astype(jnp.float32)).astype(jnp.bfloat16)
    dot = functools.partial(jnp.dot, preferred_element_type=jnp.float32)
    return dot(hi, m) + (dot(mid, m) + dot(lo, m))


def over_planes(first, last, unroll, body):
    steps = (last - first) // unroll

    def step(t, _):
        for j in range(unroll):
            body(first + t * unroll + j)
        return 0

    lax.fori_loop(0, steps, step, 0)
    for i in range(first + steps * unroll, last):
        body(i)


def interior_kernel(
    vel,
    ghost,
    visc,
    stress,
    pool_hbm,
    new_v,
    state,
    pooled,
    pool,
    coef,
    gsrc,
    ua,
    ub,
    s_sum,
    flux,
    xmat,
    sem,
):
    pool_copy = pltpu.make_async_copy(pool_hbm, pool, sem)
    pool_copy.start()
    planes = visc.shape[0] // CY
    cz = visc.shape[1]

    def at(i):
        return pl.ds(i * CY if isinstance(i, int) else pl.multiple_of(i * CY, CY), CY)

    def ghosts(c, i):
        return ghost[c, pl.ds(2 * i, 1), :], ghost[c, pl.ds(2 * i + 1, 1), :]

    def first(i):
        c, diag, scale = coefficients(visc[at(i)], visc[at(i - 1)], visc[at(i + 1)])
        for k in range(6):
            coef[k, at(i)] = c[k]
        coef[6, at(i)] = diag

        def dx(k):
            return stress[k, at(i + 1)] - stress[k, at(i - 1)]

        s_xy, s_xz, s_yz = (stress[k, at(i)] for k in (3, 4, 5))
        f = (
            dx(0) + diff_y(s_xy) + diff_z(s_xz),
            dx(3) + diff_y(stress[1, at(i)]) + diff_z(s_yz),
            dx(4) + diff_y(s_yz) + diff_z(stress[2, at(i)]),
        )
        for k in range(3):
            u = vel[k, at(i)]
            g = scale * (KAPPA * u + 0.5 * f[k])
            gsrc[k, at(i)] = g
            low, high = ghosts(k, i)
            t = gather_terms(g, c, u, vel[k, at(i - 1)], vel[k, at(i + 1)], low, high)
            ua[k, at(i)] = (1.0 - OMEGA) * u + t

    over_planes(1, planes - 1, UNROLL, first)

    def sweep(src, dst):
        def body(i):
            c = [coef[k, at(i)] for k in range(6)]
            for k in range(3):
                u = src[k, at(i)]
                low, high = ghosts(k, i)
                t = gather_terms(
                    gsrc[k, at(i)], c, u, src[k, at(i - 1)], src[k, at(i + 1)], low, high
                )
                dst[k, at(i)] = (1.0 - OMEGA) * u + t

        return body

    over_planes(2, planes - 2, UNROLL, sweep(ua, ub))
    over_planes(3, planes - 3, UNROLL, sweep(ub, new_v))

    s_sum[...] = jnp.zeros_like(s_sum)

    def residuals(b):
        for k in range(3):
            total = None
            for j in range(2):
                i = 2 * b + j
                c = [coef[n, at(i)] for n in range(6)]
                u = new_v[k, at(i)]
                low, high = ghosts(k, i)
                t = gather_terms(
                    gsrc[k, at(i)], c, u, new_v[k, at(i - 1)], new_v[k, at(i + 1)], low, high
                )
                r = (t - OMEGA * u) * coef[6, at(i)]
                total = r if total is None else total + r
            s_sum[k, at(b)] = total

    over_planes(2, planes // 2 - 2, UNROLL // 2, residuals)

    keep = lax.broadcasted_iota(jnp.int32, (planes, cz), 0)
    keep = (keep >= SWEEPS) & (keep < planes - SWEEPS)
    for k in range(3):
        for face in range(2):
            row = 0 if face == 0 else CY - 1
            nu = visc[pl.ds(row, planes, stride=CY), :]
            cell = new_v[k, pl.ds(row, planes, stride=CY), :]
            outer = ghost[k, pl.ds(face, planes, stride=2), :]
            value = nu * (cell - outer) if face == 0 else nu * (outer - cell)
            flux[...] = jnp.where(keep, value, 0.0)
            for j in range(4):
                both = flux[pl.ds(2 * j, planes // 8, stride=8), :] + flux[
                    pl.ds(2 * j + 1, planes // 8, stride=8), :
                ]
                cols = slice(j * cz, (j + 1) * cz)
                both = 0.25 * both
                first, last = k * ROWS_C + 4 + 2 * face, k * ROWS_C + HALF + 4 + face * MID
                xmat[first : first + 1, cols] = both[:1]
                xmat[first + 1 : first + 2, cols] = both[MID + 1 :]
                xmat[last : last + MID, cols] = both[1 : MID + 1]
        for j in range(4):
            both = s_sum[k, pl.ds(2 * j, planes // 2, stride=CY), :] + s_sum[
                k, pl.ds(2 * j + 1, planes // 2, stride=CY), :
            ]
            cols = slice(j * cz, (j + 1) * cz)
            xmat[k * ROWS_C : k * ROWS_C + 4, cols] = jnp.zeros((4, cz), jnp.float32)
            xmat[k * ROWS_C + 8 : k * ROWS_C + HALF + 4, cols] = 0.125 * both[2 : HALF - 2]
    pool_copy.wait()
    pooled[...] = split_dot(xmat[...], pool[...])

    for side in range(2):

        def depth(d):
            i = d if side == 0 else planes - 1 - d
            return slice(i * CY, (i + 1) * CY)

        def put(n, value):
            state[side, n * CY : (n + 1) * CY, :] = value

        for s, ref in ((1, ua), (2, ub), (3, new_v)):
            for k in range(3):
                for e in range(2):
                    put(T_U + (s - 1) * 6 + k * 2 + e, ref[k, depth(s + e), :])
        for d in range(1, 4):
            for n in range(7):
                put(T_C + n * 3 + d - 1, coef[n, depth(d), :])
            for k in range(3):
                put(T_G + k * 3 + d - 1, gsrc[k, depth(d), :])


def edge_kernel(
    n_wide,
    owner,
    mask,
    own,
    got_a,
    got_b,
    vel,
    ghost,
    visc,
    state,
    pooled,
    pool,
    velocity_in,
    velocity_out,
    *refs,
):
    slots = refs[:n_wide]
    u_out, xmat, flux, out_sem = refs[n_wide:]
    rows = velocity_out.shape[1]
    inner = pl.ds(SWEEPS * CY, rows - 2 * SWEEPS * CY)
    inner_copy = pltpu.make_async_copy(
        velocity_in.at[:, inner], velocity_out.at[:, inner], out_sem.at[2]
    )
    inner_copy.start()
    grp = lax.axis_index("grp")
    even = grp % 2 == 0
    ends = (grp > 0, grp < lax.axis_size("grp") - 1)
    cz = pool.shape[0] // 4

    me = lax.axis_index("wide")
    weights = []
    for d in range(n_wide):
        local, weight = jnp.float32(-1.0), []
        for p in range(P_SIZE):
            match = owner[0, p] // CP_DEV == me ^ d
            weight.append(jnp.where(match, mask[0, p], 0).astype(jnp.float32))
            local = jnp.where(match, (owner[0, p] % CP_DEV).astype(jnp.float32), local)
        weights.append(weight)
        slots[d][3 * ROWS_C :, :] = jnp.full((8, cz), local, jnp.float32)

    def weighted(d, value):
        total = None
        for p in range(P_SIZE):
            term = value[:, p * cz : (p + 1) * cz] * weights[d][p]
            total = term if total is None else total + term
        return total

    for k in range(3):
        part = slice(k * ROWS_C + 8, (k + 1) * ROWS_C)
        value = pooled[part, :]
        for d in range(n_wide):
            slots[d][part, :] = weighted(d, value)

    xmat[...] = jnp.zeros_like(xmat)
    flux[...] = jnp.zeros_like(flux)
    for side in range(2):
        sign = -1.0 if side == 0 else 1.0
        inside = jnp.where(ends[side], 1.0, 0.0)

        def at(d):
            i = d if side == 0 else rows // CY - 1 - d
            return slice(i * CY, (i + 1) * CY)

        def halo(r, count=CY):
            a, b = got_a[r : r + count, :], got_b[r : r + count, :]
            return jnp.where(even, b, a) if side == 0 else jnp.where(even, a, b)

        def ghosts(k, d):
            if d < 0:
                return halo(R_G + 2 * k, 1), halo(R_G + 2 * k + 1, 1)
            r = 2 * (d if side == 0 else rows // CY - 1 - d)
            return ghost[k, r : r + 1, :], ghost[k, r + 1 : r + 2, :]

        def saved(n):
            return state[side, n * CY : (n + 1) * CY, :]

        v_halo, v_own = halo(R_V), visc[at(0), :]
        coef, diag = {}, {}
        coef[-1], _, halo_scale = coefficients(v_halo, None, v_own, halo(R_N))
        coef[0], diag[0], own_scale = coefficients(v_own, v_halo, visc[at(1), :])
        for d in range(1, 4):
            c = [saved(T_C + n * 3 + d - 1) for n in range(7)]
            coef[d], diag[d] = ([c[0], c[1]] if side == 0 else [c[1], c[0]]) + c[2:6], c[6]
        for k in range(3):
            part = slice(k * CY, (k + 1) * CY)
            own_stress = own[side, (3 + k) * CY : (4 + k) * CY, :]
            g = {0: own_scale * (own[side, part, :] + (0.5 * sign) * halo(R_S + k * CY))}
            for d in range(1, 4):
                g[d] = saved(T_G + k * 3 + d - 1)
            low, high = ghosts(k, -1)
            u = {-1: halo(R_U + k * CY), 0: vel[k, at(0), :], 1: vel[k, at(1), :]}
            for s in range(1, SWEEPS + 1):
                known = halo(R_P + ((s - 1) * 3 + k) * CY) - (0.5 * sign) * own_stress
                if s == 1:
                    first = None
                elif s == 2:
                    first = u[-1]
                else:
                    known = known + halo(R_E) * first
                t = halo_scale * known + (
                    coef[-1][1] * u[0] + side_terms(coef[-1], u[-1], low, high)
                )
                new = {-1: ((1.0 - OMEGA) * u[-1] + t) * inside}
                for d in range(s):
                    t = gather_terms(g[d], coef[d], u[d], u[d - 1], u[d + 1], *ghosts(k, d))
                    new[d] = (1.0 - OMEGA) * u[d] + t
                for e in range(2):
                    new[s + e] = saved(T_U + (s - 1) * 6 + k * 2 + e)
                u = new
            for d in range(SWEEPS):
                i = d if side == 0 else SWEEPS - 1 - d
                u_out[side, k, i * CY : (i + 1) * CY, :] = u[d]
            for b in range(2):
                total = None
                for d in (2 * b, 2 * b + 1):
                    t = gather_terms(g[d], coef[d], u[d], u[d - 1], u[d + 1], *ghosts(k, d))
                    r = (t - OMEGA * u[d]) * diag[d]
                    total = r if total is None else total + r
                row = b if side == 0 else 3 - b
                both = total + pltpu.roll(total, CY - 1, 0)
                for j in range(4):
                    xmat[k * 8 + row : k * 8 + row + 1, j * cz : (j + 1) * cz] = (
                        0.125 * both[2 * j : 2 * j + 1, :]
                    )
            for d in range(SWEEPS):
                x = d if side == 0 else 7 - d
                nu = visc[at(d), :]
                low, high = ghosts(k, d)
                flux[side, k, 0, x : x + 1, :] = nu[0:1] * (u[d][0:1] - low)
                flux[side, k, 1, x : x + 1, :] = nu[CY - 1 :] * (high - u[d][CY - 1 :])
            for face in range(2):
                for j in range(4):
                    row = k * 8 + 4 + face * 2 + side
                    xmat[row : row + 1, j * cz : (j + 1) * cz] = 0.25 * (
                        flux[side, k, face, 2 * j : 2 * j + 1, :]
                        + flux[side, k, face, 2 * j + 1 : 2 * j + 2, :]
                    )
    out_copies = [
        pltpu.make_async_copy(
            u_out.at[side],
            velocity_out.at[:, pl.ds(0 if side == 0 else rows - SWEEPS * CY, SWEEPS * CY)],
            out_sem.at[side],
        )
        for side in range(2)
    ]
    for c in out_copies:
        c.start()

    edge = split_dot(xmat[...], pool[...])
    for k in range(3):
        part = slice(k * ROWS_C, k * ROWS_C + 8)
        value = pooled[part, :] + edge[k * 8 : (k + 1) * 8]
        for d in range(n_wide):
            slots[d][part, :] = weighted(d, value)
    for c in out_copies:
        c.wait()
    inner_copy.wait()


def collect_kernel(n_wide, *refs):
    slots, out = refs[:n_wide], refs[n_wide]
    cz = slots[0].shape[1]
    rows = lax.broadcasted_iota(jnp.int32, (CP_DEV, cz), 0).astype(jnp.float32)
    takes = [rows == slot[3 * ROWS_C : 3 * ROWS_C + 1, :] for slot in slots]
    for k in range(3):
        for place, n in enumerate(ROW_ORDER):
            total = None
            for take, slot in zip(takes, slots, strict=True):
                r = k * ROWS_C + place
                term = jnp.where(take, slot[r : r + 1, :], 0.0)
                total = term if total is None else total + term
            out[k, :, n * cz : (n + 1) * cz] = total


def on_device(velocity, coarse_ghost, viscosity, stress, patch_mask, coarse_owner):
    n_grp, n_wide = lax.axis_size("grp"), lax.axis_size("wide")
    cells_x, cz = viscosity.shape[0], viscosity.shape[2]
    f32 = jnp.float32
    vel = velocity.reshape(3, cells_x * CY, cz)
    ghost = coarse_ghost.reshape(3, cells_x * 2, cz)
    visc = viscosity.reshape(cells_x * CY, cz)
    strs = stress.reshape(6, cells_x * CY, cz)
    pool = jnp.asarray(pool_matrix(cz), jnp.bfloat16)

    anywhere = pl.BlockSpec(memory_space=pltpu.HBM)
    vmem = pl.BlockSpec(memory_space=pltpu.VMEM)
    smem = pl.BlockSpec(memory_space=pltpu.SMEM)
    pack_shape = jax.ShapeDtypeStruct((PACK, cz), f32)
    pack_a, pack_b, own = pl.pallas_call(
        pack_kernel,
        out_shape=(pack_shape, pack_shape, jax.ShapeDtypeStruct((2, 6 * CY, cz), f32)),
        in_specs=[anywhere] * 4,
        out_specs=(vmem, vmem, vmem),
        scratch_shapes=[
            pltpu.VMEM((2, 3, 4 * CY, cz), f32),
            pltpu.VMEM((2, 4 * CY, cz), f32),
            pltpu.VMEM((2, 6, 4 * CY, cz), f32),
            pltpu.VMEM((2, 3, 8, cz), f32),
            pltpu.SemaphoreType.DMA((2, 4)),
        ],
        compiler_params=pltpu.CompilerParams(vmem_limit_bytes=4 * 2**20),
        name="pack",
    )(*(pltpu.with_memory_space_constraint(x, pltpu.HBM) for x in (vel, ghost, visc, strs)))

    pairs_a = [(i, i ^ 1) for i in range(n_grp) if i ^ 1 < n_grp]
    pairs_b = [(i, j) for i in range(n_grp) for j in [((i + 1) ^ 1) - 1] if 0 <= j < n_grp]
    got_b = lax.ppermute(pack_b, "grp", pairs_b)
    got_a = lax.ppermute(pack_a, "grp", pairs_a)

    rows = cells_x * CY
    new_v, state, pooled, pool = pl.pallas_call(
        interior_kernel,
        out_shape=(
            jax.ShapeDtypeStruct((3, rows, cz), f32),
            jax.ShapeDtypeStruct((2, STATE * CY, cz), f32),
            jax.ShapeDtypeStruct((3 * ROWS_C, P_SIZE * cz), f32),
            jax.ShapeDtypeStruct(pool.shape, pool.dtype),
        ),
        in_specs=[vmem] * 4 + [anywhere],
        out_specs=(vmem, vmem, vmem, vmem),
        scratch_shapes=[
            pltpu.VMEM((7, rows, cz), f32),
            pltpu.VMEM((3, rows, cz), f32),
            pltpu.VMEM((3, rows, cz), f32),
            pltpu.VMEM((3, rows, cz), f32),
            pltpu.VMEM((3, rows // 2, cz), f32),
            pltpu.VMEM((cells_x, cz), f32),
            pltpu.VMEM((3 * ROWS_C, 4 * cz), f32),
            pltpu.SemaphoreType.DMA,
        ],
        cost_estimate=pl.CostEstimate(flops=100_000_000, bytes_accessed=4_000_000, transcendentals=0),
        compiler_params=pltpu.CompilerParams(vmem_limit_bytes=20 * 2**20),
        name="interior",
    )(vel, ghost, visc, strs, pltpu.with_memory_space_constraint(pool, pltpu.HBM))

    slot_shape = jax.ShapeDtypeStruct((SLOT, cz), f32)
    outs = pl.pallas_call(
        functools.partial(edge_kernel, n_wide),
        out_shape=(jax.ShapeDtypeStruct(new_v.shape, f32),) + (slot_shape,) * n_wide,
        in_specs=[smem, smem] + [vmem] * 10,
        out_specs=(anywhere,) + (vmem,) * n_wide,
        scratch_shapes=[
            pltpu.VMEM((2, 3, 3 * CY, cz), f32),
            pltpu.VMEM((24, 4 * cz), f32),
            pltpu.VMEM((2, 3, 2, 8, cz), f32),
            pltpu.SemaphoreType.DMA((3,)),
        ],
        compiler_params=pltpu.CompilerParams(vmem_limit_bytes=8 * 2**20),
        name="edge",
    )(coarse_owner, patch_mask, own, got_a, got_b, vel, ghost, visc, state, pooled, pool, new_v)
    smoothed, slots = outs[0], list(outs[1:])

    for k in range(1, n_wide):
        slots[k] = lax.ppermute(slots[k], "wide", [(i, i ^ k) for i in range(n_wide)])
    coarse = pl.pallas_call(
        functools.partial(collect_kernel, n_wide),
        out_shape=jax.ShapeDtypeStruct((3, CP_DEV, PV), f32),
        in_specs=[vmem] * n_wide,
        out_specs=vmem,
        compiler_params=pltpu.CompilerParams(vmem_limit_bytes=8 * 2**20),
        name="collect",
    )(*slots)
    return smoothed.reshape(velocity.shape), coarse.transpose(1, 0, 2)[None]


def solution(mesh):
    in_specs = (
        P(None, "grp", "wide", None),
        P(None, "grp", "wide", None),
        P("grp", "wide", None),
        P(None, "grp", "wide", None),
        P("grp", "wide"),
        P("grp", "wide"),
    )
    out_specs = (P(None, "grp", "wide", None), P("grp", "wide", None, None))
    return jax.shard_map(
        on_device, mesh=mesh, in_specs=in_specs, out_specs=out_specs, check_vma=False
    )
```

```python
import functools

import jax
import jax.numpy as jnp
import numpy as np
from jax import lax
from jax.experimental import pallas as pl
from jax.experimental.pallas import tpu as pltpu
from jax.sharding import PartitionSpec as P


PATCH = 64
CY = 8
P_SIZE = 2
CP_DEV = 16
SWEEPS = 3
PV = 6144

KAPPA = 1.0
OMEGA = 0.8

R_U = 0
R_P = 24
R_S = 96
R_V = 120
R_N = 128
R_E = 136
R_G = 144
PACK = 152

T_U = 0
T_C = 18
T_G = 39
STATE = 48

HALF = PATCH // 2
ROWS_C = HALF + 2 * (HALF // 4)
SLOT = 3 * ROWS_C + 8
UNROLL = 31
PIECES = 2

MID = HALF // 4 - 2
ROW_ORDER = (
    [0, 1, HALF - 2, HALF - 1, HALF, HALF + MID + 1, HALF + MID + 2, ROWS_C - 1]
    + list(range(2, HALF - 2))
    + list(range(HALF + 1, HALF + MID + 1))
    + list(range(HALF + MID + 3, ROWS_C - 1))
)


def pool_matrix(cz):
    k = np.arange(4 * cz)[:, None]
    n = np.arange(P_SIZE * cz)[None, :]
    same_row = (k // cz) == (n % cz) // HALF
    same_col = (k % cz) // 2 == (n // cz) * HALF + n % HALF
    return (same_row & same_col).astype(np.float32)


def up_z(v):
    return pltpu.roll(v, v.shape[1] - 1, 1)


def down_z(v):
    return pltpu.roll(v, 1, 1)


def north_of(v, high):
    row = lax.broadcasted_iota(jnp.int32, v.shape, 0)
    return jnp.where(row == CY - 1, high, pltpu.roll(v, CY - 1, 0))


def south_of(v, low):
    row = lax.broadcasted_iota(jnp.int32, v.shape, 0)
    return jnp.where(row == 0, low, pltpu.roll(v, 1, 0))


def edge_rows(v):
    row = lax.broadcasted_iota(jnp.int32, v.shape, 0)
    north = jnp.where(row == CY - 1, v, pltpu.roll(v, CY - 1, 0))
    south = jnp.where(row == 0, v, pltpu.roll(v, 1, 0))
    return north, south


def diff_y(v):
    row = lax.broadcasted_iota(jnp.int32, v.shape, 0)
    north = jnp.where(row == CY - 1, 0.0, pltpu.roll(v, CY - 1, 0))
    south = jnp.where(row == 0, 0.0, pltpu.roll(v, 1, 0))
    return north - south


def diff_z(v):
    return up_z(v) - down_z(v)


def coefficients(v, v_west, v_east, west=None):
    v_north, v_south = edge_rows(v)
    half = 0.5 * v
    east = half + 0.5 * v_east
    if west is None:
        west = half + 0.5 * v_west
    north = half + 0.5 * v_north
    south = half + 0.5 * v_south
    up = half + 0.5 * up_z(v)
    down = down_z(up)
    diagonal = KAPPA + ((east + west) + (north + south)) + (up + down)
    scale = OMEGA / diagonal
    return (
        [scale * west, scale * east, scale * south, scale * north, scale * down, scale * up],
        diagonal * (1.0 / OMEGA),
        scale,
    )


def side_terms(c, u, low, high):
    y = c[2] * south_of(u, low) + c[3] * north_of(u, high)
    z = c[4] * down_z(u) + c[5] * up_z(u)
    return y + z


def gather_terms(g, c, u, u_west, u_east, low, high):
    x = c[0] * u_west + c[1] * u_east
    return (g + x) + side_terms(c, u, low, high)


def pack_kernel(vel, ghost, visc, stress, out_a, out_b, own, u_s, v_s, s_s, g_s, sem):
    rows = vel.shape[1]
    copies = []
    for side in range(2):
        r0 = 0 if side == 0 else rows - 4 * CY
        g0 = 0 if side == 0 else ghost.shape[1] - 8
        for n, (src, dst) in enumerate(
            (
                (stress.at[:, pl.ds(r0, 4 * CY)], s_s.at[side]),
                (vel.at[:, pl.ds(r0, 4 * CY)], u_s.at[side]),
                (visc.at[pl.ds(r0, 4 * CY)], v_s.at[side]),
                (ghost.at[:, pl.ds(g0, 8)], g_s.at[side]),
            )
        ):
            copies.append(pltpu.make_async_copy(src, dst, sem.at[side, n]))
    for c in copies:
        c.start()
    for c in copies:
        c.wait()
    even = lax.axis_index("grp") % 2 == 0
    xx, yy, zz, xy, xz, yz = range(6)

    packs = []
    for side in range(2):
        sign = -1.0 if side == 0 else 1.0

        def at(d):
            p = d if side == 0 else 3 - d
            return slice(p * CY, (p + 1) * CY)

        def dx(comp, d):
            inner = s_s[side, comp, at(d + 1), :]
            return -sign * (inner - s_s[side, comp, at(d - 1), :]) if d else -sign * inner

        def ghosts(c, d):
            r = 2 * (d if side == 0 else 3 - d)
            return g_s[side, c, r : r + 1, :], g_s[side, c, r + 1 : r + 2, :]

        force = {}
        for d in range(3):
            s_xy, s_xz, s_yz, s_yy, s_zz = (s_s[side, k, at(d), :] for k in (xy, xz, yz, yy, zz))
            f = (
                dx(xx, d) + diff_y(s_xy) + diff_z(s_xz),
                dx(xy, d) + diff_y(s_yy) + diff_z(s_yz),
                dx(xz, d) + diff_y(s_yz) + diff_z(s_zz),
            )
            for c in range(3):
                force[c, d] = KAPPA * u_s[side, c, at(d), :] + 0.5 * f[c]
        v = [v_s[side, at(d), :] for d in range(4)]
        coef, scale = {}, {}
        for d in (1, 2):
            coef[d], _, scale[d] = coefficients(v[d], v[d - 1], v[d + 1])
        face = 0.5 * v[0] + 0.5 * v[1]
        parts = {R_V: v[0], R_N: face, R_E: face * coef[1][0]}
        for c, k in enumerate((xx, xy, xz)):
            u = [u_s[side, c, at(d), :] for d in range(4)]
            once = {}
            for d in (1, 2):
                low, high = ghosts(c, d)
                t = gather_terms(
                    scale[d] * force[c, d], coef[d], u[d], u[d - 1], u[d + 1], low, high
                )
                once[d] = (1.0 - OMEGA) * u[d] + t
            low, high = ghosts(c, 1)
            rest = side_terms(coef[1], once[1], low, high)
            twice = (1.0 - OMEGA) * once[1] + (
                scale[1] * force[c, 1] + coef[1][1] * once[2] + rest
            )
            for n, inner in enumerate((u[1], once[1], twice)):
                parts[R_P + (n * 3 + c) * CY] = force[c, 0] + face * inner
            parts[R_U + c * CY] = u[0]
            parts[R_S + c * CY] = s_s[side, k, at(0), :]
            own[side, c * CY : (c + 1) * CY, :] = force[c, 0]
            own[side, (3 + c) * CY : (4 + c) * CY, :] = s_s[side, k, at(0), :]
            low, high = ghosts(c, 0)
            parts[R_G + 2 * c], parts[R_G + 2 * c + 1] = low, high
        packs.append(parts)
    for r, low in packs[0].items():
        high = packs[1][r]
        out_a[r : r + low.shape[0], :] = jnp.where(even, high, low)
        out_b[r : r + low.shape[0], :] = jnp.where(even, low, high)
    for out in (out_a, out_b):
        out[R_G + 6 :, :] = jnp.zeros_like(out[R_G + 6 :, :])


def split_dot(x, m):
    hi = x.astype(jnp.bfloat16)
    rest = x - hi.astype(jnp.float32)
    mid = rest.astype(jnp.bfloat16)
    lo = (rest - mid.astype(jnp.float32)).astype(jnp.bfloat16)
    dot = functools.partial(jnp.dot, preferred_element_type=jnp.float32)
    return dot(hi, m) + (dot(mid, m) + dot(lo, m))


def over_planes(first, last, unroll, body):
    steps = (last - first) // unroll

    def step(t, _):
        for j in range(unroll):
            body(first + t * unroll + j)
        return 0

    lax.fori_loop(0, steps, step, 0)
    for i in range(first + steps * unroll, last):
        body(i)


def interior_kernel(
    vel,
    ghost,
    visc,
    stress,
    pool_hbm,
    owner_hbm,
    mask_hbm,
    new_v,
    state,
    pooled,
    pool,
    weights,
    coef,
    gsrc,
    ua,
    ub,
    s_sum,
    flux,
    xmat,
    owner,
    mask,
    sem,
):
    pool_copy = pltpu.make_async_copy(pool_hbm, pool, sem.at[0])
    owner_copy = pltpu.make_async_copy(owner_hbm, owner, sem.at[1])
    mask_copy = pltpu.make_async_copy(mask_hbm, mask, sem.at[2])
    for c in (pool_copy, owner_copy, mask_copy):
        c.start()
    planes = visc.shape[0] // CY
    cz = visc.shape[1]

    def at(i):
        return pl.ds(i * CY if isinstance(i, int) else pl.multiple_of(i * CY, CY), CY)

    def ghosts(c, i):
        return ghost[c, pl.ds(2 * i, 1), :], ghost[c, pl.ds(2 * i + 1, 1), :]

    def first(i):
        c, diag, scale = coefficients(visc[at(i)], visc[at(i - 1)], visc[at(i + 1)])
        for k in range(6):
            coef[k, at(i)] = c[k]
        coef[6, at(i)] = diag

        def dx(k):
            return stress[k, at(i + 1)] - stress[k, at(i - 1)]

        s_xy, s_xz, s_yz = (stress[k, at(i)] for k in (3, 4, 5))
        f = (
            dx(0) + diff_y(s_xy) + diff_z(s_xz),
            dx(3) + diff_y(stress[1, at(i)]) + diff_z(s_yz),
            dx(4) + diff_y(s_yz) + diff_z(stress[2, at(i)]),
        )
        for k in range(3):
            u = vel[k, at(i)]
            g = scale * (KAPPA * u + 0.5 * f[k])
            gsrc[k, at(i)] = g
            low, high = ghosts(k, i)
            t = gather_terms(g, c, u, vel[k, at(i - 1)], vel[k, at(i + 1)], low, high)
            ua[k, at(i)] = (1.0 - OMEGA) * u + t

    over_planes(1, planes - 1, UNROLL, first)

    def sweep(src, dst):
        def body(i):
            c = [coef[k, at(i)] for k in range(6)]
            for k in range(3):
                u = src[k, at(i)]
                low, high = ghosts(k, i)
                t = gather_terms(
                    gsrc[k, at(i)], c, u, src[k, at(i - 1)], src[k, at(i + 1)], low, high
                )
                dst[k, at(i)] = (1.0 - OMEGA) * u + t

        return body

    over_planes(2, planes - 2, UNROLL, sweep(ua, ub))
    over_planes(3, planes - 3, UNROLL, sweep(ub, new_v))

    s_sum[...] = jnp.zeros_like(s_sum)

    def residuals(b):
        for k in range(3):
            total = None
            for j in range(2):
                i = 2 * b + j
                c = [coef[n, at(i)] for n in range(6)]
                u = new_v[k, at(i)]
                low, high = ghosts(k, i)
                t = gather_terms(
                    gsrc[k, at(i)], c, u, new_v[k, at(i - 1)], new_v[k, at(i + 1)], low, high
                )
                r = (t - OMEGA * u) * coef[6, at(i)]
                total = r if total is None else total + r
            s_sum[k, at(b)] = total

    over_planes(2, planes // 2 - 2, UNROLL // 2, residuals)

    keep = lax.broadcasted_iota(jnp.int32, (planes, cz), 0)
    keep = (keep >= SWEEPS) & (keep < planes - SWEEPS)
    for k in range(3):
        for face in range(2):
            row = 0 if face == 0 else CY - 1
            nu = visc[pl.ds(row, planes, stride=CY), :]
            cell = new_v[k, pl.ds(row, planes, stride=CY), :]
            outer = ghost[k, pl.ds(face, planes, stride=2), :]
            value = nu * (cell - outer) if face == 0 else nu * (outer - cell)
            flux[...] = jnp.where(keep, value, 0.0)
            for j in range(4):
                both = flux[pl.ds(2 * j, planes // 8, stride=8), :] + flux[
                    pl.ds(2 * j + 1, planes // 8, stride=8), :
                ]
                cols = slice(j * cz, (j + 1) * cz)
                both = 0.25 * both
                first, last = k * ROWS_C + 4 + 2 * face, k * ROWS_C + HALF + 4 + face * MID
                xmat[first : first + 1, cols] = both[:1]
                xmat[first + 1 : first + 2, cols] = both[MID + 1 :]
                xmat[last : last + MID, cols] = both[1 : MID + 1]
        for j in range(4):
            both = s_sum[k, pl.ds(2 * j, planes // 2, stride=CY), :] + s_sum[
                k, pl.ds(2 * j + 1, planes // 2, stride=CY), :
            ]
            cols = slice(j * cz, (j + 1) * cz)
            xmat[k * ROWS_C : k * ROWS_C + 4, cols] = jnp.zeros((4, cz), jnp.float32)
            xmat[k * ROWS_C + 8 : k * ROWS_C + HALF + 4, cols] = 0.125 * both[2 : HALF - 2]
    owner_copy.wait()
    mask_copy.wait()
    me = lax.axis_index("wide")
    for d in range(weights.shape[0] // (P_SIZE + 1)):
        local = jnp.float32(-1.0)
        for p in range(P_SIZE):
            match = owner[0, p] // CP_DEV == me ^ d
            weight = jnp.where(match, mask[0, p], 0).astype(jnp.float32)
            local = jnp.where(match, (owner[0, p] % CP_DEV).astype(jnp.float32), local)
            weights[d * (P_SIZE + 1) + p] = jnp.full((8, cz), weight, jnp.float32)
        weights[d * (P_SIZE + 1) + P_SIZE] = jnp.full((8, cz), local, jnp.float32)

    pool_copy.wait()
    pooled[...] = split_dot(xmat[...], pool[...])

    for side in range(2):

        def depth(d):
            i = d if side == 0 else planes - 1 - d
            return slice(i * CY, (i + 1) * CY)

        def put(n, value):
            state[side, n * CY : (n + 1) * CY, :] = value

        for s, ref in ((1, ua), (2, ub), (3, new_v)):
            for k in range(3):
                for e in range(2):
                    put(T_U + (s - 1) * 6 + k * 2 + e, ref[k, depth(s + e), :])
        for d in range(1, 4):
            for n in range(7):
                put(T_C + n * 3 + d - 1, coef[n, depth(d), :])
            for k in range(3):
                put(T_G + k * 3 + d - 1, gsrc[k, depth(d), :])


def edge_kernel(
    n_wide,
    weights,
    own,
    got_a,
    got_b,
    vel,
    ghost,
    visc,
    state,
    pooled,
    pool,
    u_out,
    *refs,
):
    slots = refs[:n_wide]
    xmat, flux = refs[n_wide:]
    rows = visc.shape[0]
    grp = lax.axis_index("grp")
    even = grp % 2 == 0
    ends = (grp > 0, grp < lax.axis_size("grp") - 1)
    cz = pool.shape[0] // 4

    for d in range(n_wide):
        slots[d][3 * ROWS_C :, :] = weights[d * (P_SIZE + 1) + P_SIZE]

    def weighted(d, value):
        total = None
        for p in range(P_SIZE):
            term = value[:, p * cz : (p + 1) * cz] * weights[d * (P_SIZE + 1) + p, 0:1, :]
            total = term if total is None else total + term
        return total

    for k in range(3):
        part = slice(k * ROWS_C + 8, (k + 1) * ROWS_C)
        value = pooled[part, :]
        for d in range(n_wide):
            slots[d][part, :] = weighted(d, value)

    xmat[...] = jnp.zeros_like(xmat)
    flux[...] = jnp.zeros_like(flux)
    for side in range(2):
        sign = -1.0 if side == 0 else 1.0
        inside = jnp.where(ends[side], 1.0, 0.0)

        def at(d):
            i = d if side == 0 else rows // CY - 1 - d
            return slice(i * CY, (i + 1) * CY)

        def halo(r, count=CY):
            a, b = got_a[r : r + count, :], got_b[r : r + count, :]
            return jnp.where(even, b, a) if side == 0 else jnp.where(even, a, b)

        def ghosts(k, d):
            if d < 0:
                return halo(R_G + 2 * k, 1), halo(R_G + 2 * k + 1, 1)
            r = 2 * (d if side == 0 else rows // CY - 1 - d)
            return ghost[k, r : r + 1, :], ghost[k, r + 1 : r + 2, :]

        def saved(n):
            return state[side, n * CY : (n + 1) * CY, :]

        v_halo, v_own = halo(R_V), visc[at(0), :]
        coef, diag = {}, {}
        coef[-1], _, halo_scale = coefficients(v_halo, None, v_own, halo(R_N))
        coef[0], diag[0], own_scale = coefficients(v_own, v_halo, visc[at(1), :])
        for d in range(1, 4):
            c = [saved(T_C + n * 3 + d - 1) for n in range(7)]
            coef[d], diag[d] = ([c[0], c[1]] if side == 0 else [c[1], c[0]]) + c[2:6], c[6]
        for k in range(3):
            part = slice(k * CY, (k + 1) * CY)
            own_stress = own[side, (3 + k) * CY : (4 + k) * CY, :]
            g = {0: own_scale * (own[side, part, :] + (0.5 * sign) * halo(R_S + k * CY))}
            for d in range(1, 4):
                g[d] = saved(T_G + k * 3 + d - 1)
            low, high = ghosts(k, -1)
            u = {-1: halo(R_U + k * CY), 0: vel[k, at(0), :], 1: vel[k, at(1), :]}
            for s in range(1, SWEEPS + 1):
                known = halo(R_P + ((s - 1) * 3 + k) * CY) - (0.5 * sign) * own_stress
                if s == 1:
                    first = None
                elif s == 2:
                    first = u[-1]
                else:
                    known = known + halo(R_E) * first
                t = halo_scale * known + (
                    coef[-1][1] * u[0] + side_terms(coef[-1], u[-1], low, high)
                )
                new = {-1: ((1.0 - OMEGA) * u[-1] + t) * inside}
                for d in range(s):
                    t = gather_terms(g[d], coef[d], u[d], u[d - 1], u[d + 1], *ghosts(k, d))
                    new[d] = (1.0 - OMEGA) * u[d] + t
                for e in range(2):
                    new[s + e] = saved(T_U + (s - 1) * 6 + k * 2 + e)
                u = new
            for d in range(SWEEPS):
                i = d if side == 0 else SWEEPS - 1 - d
                u_out[side, k, i * CY : (i + 1) * CY, :] = u[d]
            for b in range(2):
                total = None
                for d in (2 * b, 2 * b + 1):
                    t = gather_terms(g[d], coef[d], u[d], u[d - 1], u[d + 1], *ghosts(k, d))
                    r = (t - OMEGA * u[d]) * diag[d]
                    total = r if total is None else total + r
                row = b if side == 0 else 3 - b
                both = total + pltpu.roll(total, CY - 1, 0)
                for j in range(4):
                    xmat[k * 8 + row : k * 8 + row + 1, j * cz : (j + 1) * cz] = (
                        0.125 * both[2 * j : 2 * j + 1, :]
                    )
            for d in range(SWEEPS):
                x = d if side == 0 else 7 - d
                nu = visc[at(d), :]
                low, high = ghosts(k, d)
                flux[side, k, 0, x : x + 1, :] = nu[0:1] * (u[d][0:1] - low)
                flux[side, k, 1, x : x + 1, :] = nu[CY - 1 :] * (high - u[d][CY - 1 :])
            for face in range(2):
                for j in range(4):
                    row = k * 8 + 4 + face * 2 + side
                    xmat[row : row + 1, j * cz : (j + 1) * cz] = 0.25 * (
                        flux[side, k, face, 2 * j : 2 * j + 1, :]
                        + flux[side, k, face, 2 * j + 1 : 2 * j + 2, :]
                    )
    edge = split_dot(xmat[...], pool[...])
    for k in range(3):
        part = slice(k * ROWS_C, k * ROWS_C + 8)
        value = pooled[part, :] + edge[k * 8 : (k + 1) * 8]
        for d in range(n_wide):
            slots[d][part, :] = weighted(d, value)


def velocity_kernel(inner, edges, out, sem):
    rows, rim = out.shape[1], edges.shape[2]
    mid = pl.ds(rim, rows - 2 * rim)
    copies = [
        pltpu.make_async_copy(inner.at[:, mid], out.at[:, mid], sem.at[0]),
        pltpu.make_async_copy(edges.at[0], out.at[:, pl.ds(0, rim)], sem.at[1]),
        pltpu.make_async_copy(edges.at[1], out.at[:, pl.ds(rows - rim, rim)], sem.at[2]),
    ]
    for c in copies:
        c.start()
    for c in copies:
        c.wait()


def collect_kernel(n_wide, *refs):
    slots, out, (block, sem) = refs[:n_wide], refs[n_wide], refs[n_wide + 1 :]
    cz = slots[0].shape[1]
    rows = lax.broadcasted_iota(jnp.int32, (CP_DEV, cz), 0).astype(jnp.float32)
    takes = [rows == slot[3 * ROWS_C : 3 * ROWS_C + 1, :] for slot in slots]
    width = PV // PIECES
    place_of = {n: place for place, n in enumerate(ROW_ORDER)}
    copies = []
    for k in range(3):
        for piece in range(PIECES):
            for n in range(piece * width // cz, (piece + 1) * width // cz):
                total = None
                for take, slot in zip(takes, slots, strict=True):
                    r = k * ROWS_C + place_of[n]
                    term = jnp.where(take, slot[r : r + 1, :], 0.0)
                    total = term if total is None else total + term
                block[k, :, n * cz : (n + 1) * cz] = total
            part = (k, slice(None), pl.ds(piece * width, width))
            copies.append(
                pltpu.make_async_copy(block.at[part], out.at[part], sem.at[k * PIECES + piece])
            )
            copies[-1].start()
    for c in copies:
        c.wait()


def on_device(velocity, coarse_ghost, viscosity, stress, patch_mask, coarse_owner):
    n_grp, n_wide = lax.axis_size("grp"), lax.axis_size("wide")
    cells_x, cz = viscosity.shape[0], viscosity.shape[2]
    f32 = jnp.float32
    vel = velocity.reshape(3, cells_x * CY, cz)
    ghost = coarse_ghost.reshape(3, cells_x * 2, cz)
    visc = viscosity.reshape(cells_x * CY, cz)
    strs = stress.reshape(6, cells_x * CY, cz)
    pool = jnp.asarray(pool_matrix(cz), jnp.bfloat16)

    anywhere = pl.BlockSpec(memory_space=pltpu.HBM)
    vmem = pl.BlockSpec(memory_space=pltpu.VMEM)
    pack_shape = jax.ShapeDtypeStruct((PACK, cz), f32)
    pack_a, pack_b, own = pl.pallas_call(
        pack_kernel,
        out_shape=(pack_shape, pack_shape, jax.ShapeDtypeStruct((2, 6 * CY, cz), f32)),
        in_specs=[anywhere] * 4,
        out_specs=(vmem, vmem, vmem),
        scratch_shapes=[
            pltpu.VMEM((2, 3, 4 * CY, cz), f32),
            pltpu.VMEM((2, 4 * CY, cz), f32),
            pltpu.VMEM((2, 6, 4 * CY, cz), f32),
            pltpu.VMEM((2, 3, 8, cz), f32),
            pltpu.SemaphoreType.DMA((2, 4)),
        ],
        compiler_params=pltpu.CompilerParams(vmem_limit_bytes=4 * 2**20),
        name="pack",
    )(*(pltpu.with_memory_space_constraint(x, pltpu.HBM) for x in (vel, ghost, visc, strs)))

    pairs_a = [(i, i ^ 1) for i in range(n_grp) if i ^ 1 < n_grp]
    pairs_b = [(i, j) for i in range(n_grp) for j in [((i + 1) ^ 1) - 1] if 0 <= j < n_grp]
    got_b = lax.ppermute(pack_b, "grp", pairs_b)
    got_a = lax.ppermute(pack_a, "grp", pairs_a)

    rows = cells_x * CY
    new_v, state, pooled, pool, weights = pl.pallas_call(
        interior_kernel,
        out_shape=(
            jax.ShapeDtypeStruct((3, rows, cz), f32),
            jax.ShapeDtypeStruct((2, STATE * CY, cz), f32),
            jax.ShapeDtypeStruct((3 * ROWS_C, P_SIZE * cz), f32),
            jax.ShapeDtypeStruct(pool.shape, pool.dtype),
            jax.ShapeDtypeStruct((n_wide * (P_SIZE + 1), 8, cz), f32),
        ),
        in_specs=[vmem] * 4 + [anywhere] * 3,
        out_specs=(vmem,) * 5,
        scratch_shapes=[
            pltpu.VMEM((7, rows, cz), f32),
            pltpu.VMEM((3, rows, cz), f32),
            pltpu.VMEM((3, rows, cz), f32),
            pltpu.VMEM((3, rows, cz), f32),
            pltpu.VMEM((3, rows // 2, cz), f32),
            pltpu.VMEM((cells_x, cz), f32),
            pltpu.VMEM((3 * ROWS_C, 4 * cz), f32),
            pltpu.SMEM((1, P_SIZE), jnp.int32),
            pltpu.SMEM((1, P_SIZE), jnp.int32),
            pltpu.SemaphoreType.DMA((3,)),
        ],
        cost_estimate=pl.CostEstimate(flops=100_000_000, bytes_accessed=4_000_000, transcendentals=0),
        compiler_params=pltpu.CompilerParams(vmem_limit_bytes=20 * 2**20),
        name="interior",
    )(
        vel,
        ghost,
        visc,
        strs,
        *(pltpu.with_memory_space_constraint(x, pltpu.HBM) for x in (pool, coarse_owner, patch_mask)),
    )

    slot_shape = jax.ShapeDtypeStruct((SLOT, cz), f32)
    rim_shape = jax.ShapeDtypeStruct((2, 3, SWEEPS * CY, cz), f32)
    outs = pl.pallas_call(
        functools.partial(edge_kernel, n_wide),
        out_shape=(rim_shape,) + (slot_shape,) * n_wide,
        in_specs=[vmem] * 10,
        out_specs=(vmem,) * (1 + n_wide),
        scratch_shapes=[
            pltpu.VMEM((24, 4 * cz), f32),
            pltpu.VMEM((2, 3, 2, 8, cz), f32),
        ],
        compiler_params=pltpu.CompilerParams(vmem_limit_bytes=8 * 2**20),
        name="edge",
    )(weights, own, got_a, got_b, vel, ghost, visc, state, pooled, pool)
    slots = list(outs[1:])
    smoothed = pl.pallas_call(
        velocity_kernel,
        out_shape=jax.ShapeDtypeStruct(new_v.shape, f32),
        in_specs=[vmem, vmem],
        out_specs=anywhere,
        scratch_shapes=[pltpu.SemaphoreType.DMA((3,))],
        cost_estimate=pl.CostEstimate(flops=20_000_000, bytes_accessed=1_600_000, transcendentals=0),
        compiler_params=pltpu.CompilerParams(vmem_limit_bytes=4 * 2**20),
        name="velocity",
    )(new_v, outs[0])

    for k in range(1, n_wide):
        slots[k] = lax.ppermute(slots[k], "wide", [(i, i ^ k) for i in range(n_wide)])
    coarse = pl.pallas_call(
        functools.partial(collect_kernel, n_wide),
        out_shape=jax.ShapeDtypeStruct((3, CP_DEV, PV), f32),
        in_specs=[vmem] * n_wide,
        out_specs=anywhere,
        scratch_shapes=[
            pltpu.VMEM((3, CP_DEV, PV), f32),
            pltpu.SemaphoreType.DMA((3 * PIECES,)),
        ],
        compiler_params=pltpu.CompilerParams(vmem_limit_bytes=8 * 2**20),
        name="collect",
    )(*slots)
    return smoothed.reshape(velocity.shape), coarse.transpose(1, 0, 2)[None]


def solution(mesh):
    in_specs = (
        P(None, "grp", "wide", None),
        P(None, "grp", "wide", None),
        P("grp", "wide", None),
        P(None, "grp", "wide", None),
        P("grp", "wide"),
        P("grp", "wide"),
    )
    out_specs = (P(None, "grp", "wide", None), P("grp", "wide", None, None))
    return jax.shard_map(
        on_device, mesh=mesh, in_specs=in_specs, out_specs=out_specs, check_vma=False
    )
```

```python
import functools

import jax
import jax.numpy as jnp
import numpy as np
from jax import lax
from jax.experimental import pallas as pl
from jax.experimental.pallas import tpu as pltpu
from jax.sharding import PartitionSpec as P


PATCH = 64
CY = 8
P_SIZE = 2
CP_DEV = 16
SWEEPS = 3
PV = 6144

KAPPA = 1.0
OMEGA = 0.8

R_U = 0
R_P = 24
R_S = 96
R_V = 120
R_N = 128
R_E = 136
R_G = 144
PACK = 152

T_U = 0
T_C = 18
T_G = 39
STATE = 48

HALF = PATCH // 2
ROWS_C = HALF + 2 * (HALF // 4)
EDGE = 8
LATE = 3 * EDGE + 8
EARLY = 3 * (ROWS_C - EDGE)
UNROLL = 62
PIECES = 1

MID = HALF // 4 - 2
ROW_ORDER = (
    [0, 1, HALF - 2, HALF - 1, HALF, HALF + MID + 1, HALF + MID + 2, ROWS_C - 1]
    + list(range(2, HALF - 2))
    + list(range(HALF + 1, HALF + MID + 1))
    + list(range(HALF + MID + 3, ROWS_C - 1))
)


def pool_matrix(cz):
    k = np.arange(4 * cz)[:, None]
    n = np.arange(P_SIZE * cz)[None, :]
    same_row = (k // cz) == (n % cz) // HALF
    same_col = (k % cz) // 2 == (n // cz) * HALF + n % HALF
    return (same_row & same_col).astype(np.float32)


def up_z(v):
    return pltpu.roll(v, v.shape[1] - 1, 1)


def down_z(v):
    return pltpu.roll(v, 1, 1)


def north_of(v, high):
    row = lax.broadcasted_iota(jnp.int32, v.shape, 0)
    return jnp.where(row == CY - 1, high, pltpu.roll(v, CY - 1, 0))


def south_of(v, low):
    row = lax.broadcasted_iota(jnp.int32, v.shape, 0)
    return jnp.where(row == 0, low, pltpu.roll(v, 1, 0))


def edge_rows(v):
    row = lax.broadcasted_iota(jnp.int32, v.shape, 0)
    north = jnp.where(row == CY - 1, v, pltpu.roll(v, CY - 1, 0))
    south = jnp.where(row == 0, v, pltpu.roll(v, 1, 0))
    return north, south


def diff_y(v):
    row = lax.broadcasted_iota(jnp.int32, v.shape, 0)
    north = jnp.where(row == CY - 1, 0.0, pltpu.roll(v, CY - 1, 0))
    south = jnp.where(row == 0, 0.0, pltpu.roll(v, 1, 0))
    return north - south


def diff_z(v):
    return up_z(v) - down_z(v)


def coefficients(v, v_west, v_east, west=None):
    v_north, v_south = edge_rows(v)
    east = v + v_east
    west = v + v_west if west is None else west + west
    north = v + v_north
    south = v + v_south
    up = v + up_z(v)
    down = down_z(up)
    diagonal = KAPPA + 0.5 * (((east + west) + (north + south)) + (up + down))
    scale = (0.5 * OMEGA) / diagonal
    return (
        [scale * west, scale * east, scale * south, scale * north, scale * down, scale * up],
        diagonal * (1.0 / OMEGA),
        scale,
    )


def fold_ghosts(c):
    row = lax.broadcasted_iota(jnp.int32, c[0].shape, 0)
    first, last = row == 0, row == CY - 1
    south, north = jnp.where(first, 0.0, c[2]), jnp.where(last, 0.0, c[3])
    ghost = jnp.where(first, c[2], jnp.where(last, c[3], 0.0))
    return [c[0], c[1], south, north, c[4], c[5]], ghost, first


def folded_terms(g, c, u, u_west, u_east):
    x = c[0] * u_west + c[1] * u_east
    y = c[2] * pltpu.roll(u, 1, 0) + c[3] * pltpu.roll(u, CY - 1, 0)
    z = c[4] * down_z(u) + c[5] * up_z(u)
    return (g + x) + (y + z)


def side_terms(c, u, low, high):
    y = c[2] * south_of(u, low) + c[3] * north_of(u, high)
    z = c[4] * down_z(u) + c[5] * up_z(u)
    return y + z


def gather_terms(g, c, u, u_west, u_east, low, high):
    x = c[0] * u_west + c[1] * u_east
    return (g + x) + side_terms(c, u, low, high)


def pack_kernel(vel, ghost, visc, stress, out_a, out_b, own, u_s, v_s, s_s, g_s, sem):
    rows = vel.shape[1]
    copies = []
    for side in range(2):
        r0 = 0 if side == 0 else rows - 4 * CY
        g0 = 0 if side == 0 else ghost.shape[1] - 8
        for n, (src, dst) in enumerate(
            (
                (stress.at[:, pl.ds(r0, 4 * CY)], s_s.at[side]),
                (vel.at[:, pl.ds(r0, 4 * CY)], u_s.at[side]),
                (visc.at[pl.ds(r0, 4 * CY)], v_s.at[side]),
                (ghost.at[:, pl.ds(g0, 8)], g_s.at[side]),
            )
        ):
            copies.append(pltpu.make_async_copy(src, dst, sem.at[side, n]))
    for c in copies:
        c.start()
    for c in copies:
        c.wait()
    even = lax.axis_index("grp") % 2 == 0
    xx, yy, zz, xy, xz, yz = range(6)

    packs = []
    for side in range(2):
        sign = -1.0 if side == 0 else 1.0

        def at(d):
            p = d if side == 0 else 3 - d
            return slice(p * CY, (p + 1) * CY)

        def dx(comp, d):
            inner = s_s[side, comp, at(d + 1), :]
            return -sign * (inner - s_s[side, comp, at(d - 1), :]) if d else -sign * inner

        def ghosts(c, d):
            r = 2 * (d if side == 0 else 3 - d)
            return g_s[side, c, r : r + 1, :], g_s[side, c, r + 1 : r + 2, :]

        force = {}
        for d in range(3):
            s_xy, s_xz, s_yz, s_yy, s_zz = (s_s[side, k, at(d), :] for k in (xy, xz, yz, yy, zz))
            f = (
                dx(xx, d) + diff_y(s_xy) + diff_z(s_xz),
                dx(xy, d) + diff_y(s_yy) + diff_z(s_yz),
                dx(xz, d) + diff_y(s_yz) + diff_z(s_zz),
            )
            for c in range(3):
                force[c, d] = KAPPA * u_s[side, c, at(d), :] + 0.5 * f[c]
        v = [v_s[side, at(d), :] for d in range(4)]
        coef, scale = {}, {}
        for d in (1, 2):
            coef[d], _, scale[d] = coefficients(v[d], v[d - 1], v[d + 1])
        face = 0.5 * v[0] + 0.5 * v[1]
        parts = {R_V: v[0], R_N: face, R_E: face * coef[1][0]}
        for c, k in enumerate((xx, xy, xz)):
            u = [u_s[side, c, at(d), :] for d in range(4)]
            once = {}
            for d in (1, 2):
                low, high = ghosts(c, d)
                t = gather_terms(
                    2.0 * scale[d] * force[c, d], coef[d], u[d], u[d - 1], u[d + 1], low, high
                )
                once[d] = (1.0 - OMEGA) * u[d] + t
            low, high = ghosts(c, 1)
            rest = side_terms(coef[1], once[1], low, high)
            twice = (1.0 - OMEGA) * once[1] + (
                2.0 * scale[1] * force[c, 1] + coef[1][1] * once[2] + rest
            )
            for n, inner in enumerate((u[1], once[1], twice)):
                parts[R_P + (n * 3 + c) * CY] = force[c, 0] + face * inner
            parts[R_U + c * CY] = u[0]
            parts[R_S + c * CY] = s_s[side, k, at(0), :]
            own[side, c * CY : (c + 1) * CY, :] = force[c, 0]
            own[side, (3 + c) * CY : (4 + c) * CY, :] = s_s[side, k, at(0), :]
            low, high = ghosts(c, 0)
            parts[R_G + 2 * c], parts[R_G + 2 * c + 1] = low, high
        packs.append(parts)
    for r, low in packs[0].items():
        high = packs[1][r]
        out_a[r : r + low.shape[0], :] = jnp.where(even, high, low)
        out_b[r : r + low.shape[0], :] = jnp.where(even, low, high)
    for out in (out_a, out_b):
        out[R_G + 6 :, :] = jnp.zeros_like(out[R_G + 6 :, :])


def split_dot(x, m):
    hi = x.astype(jnp.bfloat16)
    rest = x - hi.astype(jnp.float32)
    mid = rest.astype(jnp.bfloat16)
    lo = (rest - mid.astype(jnp.float32)).astype(jnp.bfloat16)
    dot = functools.partial(jnp.dot, preferred_element_type=jnp.float32)
    return dot(hi, m) + (dot(mid, m) + dot(lo, m))


def over_planes(first, last, unroll, body):
    steps = (last - first) // unroll

    def step(t, _):
        for j in range(unroll):
            body(first + t * unroll + j)
        return 0

    lax.fori_loop(0, steps, step, 0)
    for i in range(first + steps * unroll, last):
        body(i)


def weighted(weights, d, value):
    cz = weights.shape[2]
    total = None
    for p in range(P_SIZE):
        term = value[:, p * cz : (p + 1) * cz] * weights[d * (P_SIZE + 1) + p, 0:1, :]
        total = term if total is None else total + term
    return total


def interior_kernel(n_wide, vel, ghost, visc, stress, pool_hbm, owner_hbm, mask_hbm, *refs):
    new_v, state, pooled, pool, weights = refs[:5]
    early = refs[5 : 5 + n_wide // 2]
    coef, gsrc, ua, ub, s_sum, flux, xmat, owner, mask, sem = refs[5 + n_wide // 2 :]
    pool_copy = pltpu.make_async_copy(pool_hbm, pool, sem.at[0])
    owner_copy = pltpu.make_async_copy(owner_hbm, owner, sem.at[1])
    mask_copy = pltpu.make_async_copy(mask_hbm, mask, sem.at[2])
    for c in (pool_copy, owner_copy, mask_copy):
        c.start()
    planes = visc.shape[0] // CY
    cz = visc.shape[1]

    def at(i):
        return pl.ds(i * CY if isinstance(i, int) else pl.multiple_of(i * CY, CY), CY)

    def ghosts(c, i):
        return ghost[c, pl.ds(2 * i, 1), :], ghost[c, pl.ds(2 * i + 1, 1), :]

    def first(i):
        c, diag, scale = coefficients(visc[at(i)], visc[at(i - 1)], visc[at(i + 1)])
        c, c_ghost, low_row = fold_ghosts(c)
        for k in range(6):
            coef[k, at(i)] = c[k]
        coef[6, at(i)] = diag

        def dx(k):
            return stress[k, at(i + 1)] - stress[k, at(i - 1)]

        s_xy, s_xz, s_yz = (stress[k, at(i)] for k in (3, 4, 5))
        f = (
            dx(0) + diff_y(s_xy) + diff_z(s_xz),
            dx(3) + diff_y(stress[1, at(i)]) + diff_z(s_yz),
            dx(4) + diff_y(s_yz) + diff_z(stress[2, at(i)]),
        )
        for k in range(3):
            u = vel[k, at(i)]
            low, high = ghosts(k, i)
            g = scale * ((2.0 * KAPPA) * u + f[k]) + c_ghost * jnp.where(low_row, low, high)
            gsrc[k, at(i)] = g
            t = folded_terms(g, c, u, vel[k, at(i - 1)], vel[k, at(i + 1)])
            ua[k, at(i)] = (1.0 - OMEGA) * u + t

    over_planes(1, planes - 1, UNROLL, first)

    def sweep(src, dst):
        def body(i):
            c = [coef[k, at(i)] for k in range(6)]
            for k in range(3):
                u = src[k, at(i)]
                t = folded_terms(gsrc[k, at(i)], c, u, src[k, at(i - 1)], src[k, at(i + 1)])
                dst[k, at(i)] = (1.0 - OMEGA) * u + t

        return body

    over_planes(2, planes - 2, UNROLL, sweep(ua, ub))
    over_planes(3, planes - 3, UNROLL, sweep(ub, new_v))

    s_sum[...] = jnp.zeros_like(s_sum)

    def residuals(b):
        total = [None] * 3
        for j in range(2):
            i = 2 * b + j
            c = [coef[n, at(i)] for n in range(7)]
            for k in range(3):
                u = new_v[k, at(i)]
                t = folded_terms(gsrc[k, at(i)], c, u, new_v[k, at(i - 1)], new_v[k, at(i + 1)])
                r = (t - OMEGA * u) * c[6]
                total[k] = r if total[k] is None else total[k] + r
        for k in range(3):
            s_sum[k, at(b)] = total[k]

    over_planes(2, planes // 2 - 2, UNROLL // 2, residuals)

    keep = lax.broadcasted_iota(jnp.int32, (planes, cz), 0)
    keep = (keep >= SWEEPS) & (keep < planes - SWEEPS)
    for k in range(3):
        for face in range(2):
            row = 0 if face == 0 else CY - 1
            nu = visc[pl.ds(row, planes, stride=CY), :]
            cell = new_v[k, pl.ds(row, planes, stride=CY), :]
            outer = ghost[k, pl.ds(face, planes, stride=2), :]
            value = nu * (cell - outer) if face == 0 else nu * (outer - cell)
            flux[...] = jnp.where(keep, value, 0.0)
            for j in range(4):
                both = flux[pl.ds(2 * j, planes // 8, stride=8), :] + flux[
                    pl.ds(2 * j + 1, planes // 8, stride=8), :
                ]
                cols = slice(j * cz, (j + 1) * cz)
                both = 0.25 * both
                first, last = k * ROWS_C + 4 + 2 * face, k * ROWS_C + HALF + 4 + face * MID
                xmat[first : first + 1, cols] = both[:1]
                xmat[first + 1 : first + 2, cols] = both[MID + 1 :]
                xmat[last : last + MID, cols] = both[1 : MID + 1]
        for j in range(4):
            both = s_sum[k, pl.ds(2 * j, planes // 2, stride=CY), :] + s_sum[
                k, pl.ds(2 * j + 1, planes // 2, stride=CY), :
            ]
            cols = slice(j * cz, (j + 1) * cz)
            xmat[k * ROWS_C : k * ROWS_C + 4, cols] = jnp.zeros((4, cz), jnp.float32)
            xmat[k * ROWS_C + 8 : k * ROWS_C + HALF + 4, cols] = 0.125 * both[2 : HALF - 2]
    owner_copy.wait()
    mask_copy.wait()
    me = lax.axis_index("wide")
    for d in range(n_wide):
        local = jnp.float32(-1.0)
        for p in range(P_SIZE):
            match = owner[0, p] // CP_DEV == me ^ d
            weight = jnp.where(match, mask[0, p], 0).astype(jnp.float32)
            local = jnp.where(match, (owner[0, p] % CP_DEV).astype(jnp.float32), local)
            weights[d * (P_SIZE + 1) + p] = jnp.full((8, cz), weight, jnp.float32)
        weights[d * (P_SIZE + 1) + P_SIZE] = jnp.full((8, cz), local, jnp.float32)

    pool_copy.wait()
    values = split_dot(xmat[...], pool[...])
    for k in range(3):
        first, last = k * ROWS_C, (k + 1) * ROWS_C
        pooled[k * EDGE : (k + 1) * EDGE, :] = values[first : first + EDGE]
        for d in range(n_wide):
            row = d % 2 * EARLY + k * (ROWS_C - EDGE)
            early[d // 2][row : row + ROWS_C - EDGE, :] = weighted(
                weights, d, values[first + EDGE : last]
            )

    for side in range(2):

        def depth(d):
            i = d if side == 0 else planes - 1 - d
            return slice(i * CY, (i + 1) * CY)

        def put(n, value):
            state[side, n * CY : (n + 1) * CY, :] = value

        for s, ref in ((1, ua), (2, ub), (3, new_v)):
            for k in range(3):
                for e in range(2):
                    put(T_U + (s - 1) * 6 + k * 2 + e, ref[k, depth(s + e), :])
        for d in range(1, 4):
            for n in range(7):
                put(T_C + n * 3 + d - 1, coef[n, depth(d), :])
            for k in range(3):
                put(T_G + k * 3 + d - 1, gsrc[k, depth(d), :])


def edge_kernel(
    n_wide,
    weights,
    own,
    got_a,
    got_b,
    vel,
    ghost,
    visc,
    state,
    pooled,
    pool,
    early_next,
    u_out,
    *refs,
):
    late = refs[:n_wide]
    xmat, flux = refs[n_wide:]
    rows = visc.shape[0]
    grp = lax.axis_index("grp")
    even = grp % 2 == 0
    ends = (grp > 0, grp < lax.axis_size("grp") - 1)
    cz = pool.shape[0] // 4

    for d in range(n_wide):
        late[d][3 * EDGE : LATE, :] = weights[d * (P_SIZE + 1) + P_SIZE]
    late[1][LATE:, :] = early_next[EARLY:, :]

    xmat[...] = jnp.zeros_like(xmat)
    flux[...] = jnp.zeros_like(flux)
    for side in range(2):
        sign = -1.0 if side == 0 else 1.0
        inside = jnp.where(ends[side], 1.0, 0.0)

        def at(d):
            i = d if side == 0 else rows // CY - 1 - d
            return slice(i * CY, (i + 1) * CY)

        def halo(r, count=CY):
            a, b = got_a[r : r + count, :], got_b[r : r + count, :]
            return jnp.where(even, b, a) if side == 0 else jnp.where(even, a, b)

        def ghosts(k, d):
            if d < 0:
                return halo(R_G + 2 * k, 1), halo(R_G + 2 * k + 1, 1)
            r = 2 * (d if side == 0 else rows // CY - 1 - d)
            return ghost[k, r : r + 1, :], ghost[k, r + 1 : r + 2, :]

        def saved(n):
            return state[side, n * CY : (n + 1) * CY, :]

        v_halo, v_own = halo(R_V), visc[at(0), :]
        coef, diag = {}, {}
        coef[-1], _, halo_scale = coefficients(v_halo, None, v_own, halo(R_N))
        coef[0], diag[0], own_scale = coefficients(v_own, v_halo, visc[at(1), :])
        for d in range(1, 4):
            c = [saved(T_C + n * 3 + d - 1) for n in range(7)]
            coef[d], diag[d] = ([c[0], c[1]] if side == 0 else [c[1], c[0]]) + c[2:6], c[6]
        for k in range(3):
            part = slice(k * CY, (k + 1) * CY)
            own_stress = own[side, (3 + k) * CY : (4 + k) * CY, :]
            force = own[side, part, :] + (0.5 * sign) * halo(R_S + k * CY)
            g = {0: 2.0 * own_scale * force}
            for d in range(1, 4):
                g[d] = saved(T_G + k * 3 + d - 1)

            def terms(d):
                if d:
                    return folded_terms(g[d], coef[d], u[d], u[d - 1], u[d + 1])
                return gather_terms(g[d], coef[d], u[d], u[d - 1], u[d + 1], *ghosts(k, d))

            low, high = ghosts(k, -1)
            u = {-1: halo(R_U + k * CY), 0: vel[k, at(0), :], 1: vel[k, at(1), :]}
            for s in range(1, SWEEPS + 1):
                known = halo(R_P + ((s - 1) * 3 + k) * CY) - (0.5 * sign) * own_stress
                if s == 1:
                    first = None
                elif s == 2:
                    first = u[-1]
                else:
                    known = known + halo(R_E) * first
                t = 2.0 * halo_scale * known + (
                    coef[-1][1] * u[0] + side_terms(coef[-1], u[-1], low, high)
                )
                new = {-1: ((1.0 - OMEGA) * u[-1] + t) * inside}
                for d in range(s):
                    t = terms(d)
                    new[d] = (1.0 - OMEGA) * u[d] + t
                for e in range(2):
                    new[s + e] = saved(T_U + (s - 1) * 6 + k * 2 + e)
                u = new
            for d in range(SWEEPS):
                i = d if side == 0 else SWEEPS - 1 - d
                u_out[side, k, i * CY : (i + 1) * CY, :] = u[d]
            for b in range(2):
                total = None
                for d in (2 * b, 2 * b + 1):
                    t = terms(d)
                    r = (t - OMEGA * u[d]) * diag[d]
                    total = r if total is None else total + r
                row = b if side == 0 else 3 - b
                both = total + pltpu.roll(total, CY - 1, 0)
                for j in range(4):
                    xmat[k * 8 + row : k * 8 + row + 1, j * cz : (j + 1) * cz] = (
                        0.125 * both[2 * j : 2 * j + 1, :]
                    )
            for d in range(SWEEPS):
                x = d if side == 0 else 7 - d
                nu = visc[at(d), :]
                low, high = ghosts(k, d)
                flux[side, k, 0, x : x + 1, :] = nu[0:1] * (u[d][0:1] - low)
                flux[side, k, 1, x : x + 1, :] = nu[CY - 1 :] * (high - u[d][CY - 1 :])
            for face in range(2):
                for j in range(4):
                    row = k * 8 + 4 + face * 2 + side
                    xmat[row : row + 1, j * cz : (j + 1) * cz] = 0.25 * (
                        flux[side, k, face, 2 * j : 2 * j + 1, :]
                        + flux[side, k, face, 2 * j + 1 : 2 * j + 2, :]
                    )
    edge = pooled[...] + split_dot(xmat[...], pool[...])
    for d in range(n_wide):
        late[d][0 : 3 * EDGE, :] = weighted(weights, d, edge)


def velocity_kernel(inner, edges, out, sem):
    rows, rim = out.shape[1], edges.shape[2]
    mid = pl.ds(rim, rows - 2 * rim)
    copies = [
        pltpu.make_async_copy(inner.at[:, mid], out.at[:, mid], sem.at[0]),
        pltpu.make_async_copy(edges.at[0], out.at[:, pl.ds(0, rim)], sem.at[1]),
        pltpu.make_async_copy(edges.at[1], out.at[:, pl.ds(rows - rim, rim)], sem.at[2]),
    ]
    for c in copies:
        c.start()
    for c in copies:
        c.wait()


def collect_kernel(n_wide, *refs):
    late = refs[:n_wide]
    early = [refs[n_wide], late[1]] + list(refs[n_wide + 1 : 2 * n_wide - 1])
    starts = [LATE if d == 1 else d % 2 * EARLY for d in range(n_wide)]
    out, block, sem = refs[2 * n_wide - 1 :]
    cz = late[0].shape[1]
    rows = lax.broadcasted_iota(jnp.int32, (CP_DEV, cz), 0).astype(jnp.float32)
    takes = [rows == slot[3 * EDGE : 3 * EDGE + 1, :] for slot in late]
    width = PV // PIECES
    place_of = {n: place for place, n in enumerate(ROW_ORDER)}
    copies = []
    for k in range(3):
        for piece in range(PIECES):
            for n in range(piece * width // cz, (piece + 1) * width // cz):
                total = None
                for d, take in enumerate(takes):
                    if place_of[n] < EDGE:
                        slot, r = late[d], k * EDGE + place_of[n]
                    else:
                        slot, r = early[d], starts[d] + k * (ROWS_C - EDGE) + place_of[n] - EDGE
                    term = jnp.where(take, slot[r : r + 1, :], 0.0)
                    total = term if total is None else total + term
                block[k, :, n * cz : (n + 1) * cz] = total
            part = (k, slice(None), pl.ds(piece * width, width))
            copies.append(
                pltpu.make_async_copy(block.at[part], out.at[part], sem.at[k * PIECES + piece])
            )
            copies[-1].start()
    for c in copies:
        c.wait()


def on_device(velocity, coarse_ghost, viscosity, stress, patch_mask, coarse_owner):
    n_grp, n_wide = lax.axis_size("grp"), lax.axis_size("wide")
    cells_x, cz = viscosity.shape[0], viscosity.shape[2]
    f32 = jnp.float32
    vel = velocity.reshape(3, cells_x * CY, cz)
    ghost = coarse_ghost.reshape(3, cells_x * 2, cz)
    visc = viscosity.reshape(cells_x * CY, cz)
    strs = stress.reshape(6, cells_x * CY, cz)
    pool = jnp.asarray(pool_matrix(cz), jnp.bfloat16)

    anywhere = pl.BlockSpec(memory_space=pltpu.HBM)
    vmem = pl.BlockSpec(memory_space=pltpu.VMEM)
    pack_shape = jax.ShapeDtypeStruct((PACK, cz), f32)
    pack_a, pack_b, own = pl.pallas_call(
        pack_kernel,
        out_shape=(pack_shape, pack_shape, jax.ShapeDtypeStruct((2, 6 * CY, cz), f32)),
        in_specs=[anywhere] * 4,
        out_specs=(vmem, vmem, vmem),
        scratch_shapes=[
            pltpu.VMEM((2, 3, 4 * CY, cz), f32),
            pltpu.VMEM((2, 4 * CY, cz), f32),
            pltpu.VMEM((2, 6, 4 * CY, cz), f32),
            pltpu.VMEM((2, 3, 8, cz), f32),
            pltpu.SemaphoreType.DMA((2, 4)),
        ],
        compiler_params=pltpu.CompilerParams(vmem_limit_bytes=4 * 2**20),
        name="pack",
    )(*(pltpu.with_memory_space_constraint(x, pltpu.HBM) for x in (vel, ghost, visc, strs)))

    pairs_a = [(i, i ^ 1) for i in range(n_grp) if i ^ 1 < n_grp]
    pairs_b = [(i, j) for i in range(n_grp) for j in [((i + 1) ^ 1) - 1] if 0 <= j < n_grp]
    got_a = lax.ppermute(pack_a, "grp", pairs_a)
    got_b = lax.ppermute(pack_b, "grp", pairs_b)

    rows = cells_x * CY
    interior = pl.pallas_call(
        functools.partial(interior_kernel, n_wide),
        out_shape=(
            jax.ShapeDtypeStruct((3, rows, cz), f32),
            jax.ShapeDtypeStruct((2, STATE * CY, cz), f32),
            jax.ShapeDtypeStruct((3 * EDGE, P_SIZE * cz), f32),
            jax.ShapeDtypeStruct(pool.shape, pool.dtype),
            jax.ShapeDtypeStruct((n_wide * (P_SIZE + 1), 8, cz), f32),
        )
        + (jax.ShapeDtypeStruct((2 * EARLY, cz), f32),) * (n_wide // 2),
        in_specs=[vmem] * 4 + [anywhere] * 3,
        out_specs=(vmem,) * (5 + n_wide // 2),
        scratch_shapes=[
            pltpu.VMEM((7, rows, cz), f32),
            pltpu.VMEM((3, rows, cz), f32),
            pltpu.VMEM((3, rows, cz), f32),
            pltpu.VMEM((3, rows, cz), f32),
            pltpu.VMEM((3, rows // 2, cz), f32),
            pltpu.VMEM((cells_x, cz), f32),
            pltpu.VMEM((3 * ROWS_C, 4 * cz), f32),
            pltpu.SMEM((1, P_SIZE), jnp.int32),
            pltpu.SMEM((1, P_SIZE), jnp.int32),
            pltpu.SemaphoreType.DMA((3,)),
        ],
        cost_estimate=pl.CostEstimate(flops=100_000_000, bytes_accessed=4_000_000, transcendentals=0),
        compiler_params=pltpu.CompilerParams(vmem_limit_bytes=20 * 2**20),
        name="interior",
    )
    new_v, state, pooled, pool, weights, *early = interior(
        vel,
        ghost,
        visc,
        strs,
        *(
            pltpu.with_memory_space_constraint(x, pltpu.HBM)
            for x in (pool, coarse_owner, patch_mask)
        ),
    )

    def send(x, k):
        return lax.ppermute(x, "wide", [(i, i ^ k) for i in range(n_wide)])

    pairs = {}
    for k in range(2, n_wide, 2):
        pairs[k] = send(early[k // 2], k)

    rim_shape = jax.ShapeDtypeStruct((2, 3, SWEEPS * CY, cz), f32)
    outs = pl.pallas_call(
        functools.partial(edge_kernel, n_wide),
        out_shape=(rim_shape,)
        + tuple(
            jax.ShapeDtypeStruct((LATE + (EARLY if d == 1 else 0), cz), f32) for d in range(n_wide)
        ),
        in_specs=[vmem] * 11,
        out_specs=(vmem,) * (1 + n_wide),
        scratch_shapes=[
            pltpu.VMEM((24, 4 * cz), f32),
            pltpu.VMEM((2, 3, 2, 8, cz), f32),
        ],
        compiler_params=pltpu.CompilerParams(vmem_limit_bytes=8 * 2**20),
        name="edge",
    )(weights, own, got_a, got_b, vel, ghost, visc, state, pooled, pool, early[0])
    late = list(outs[1:])
    smoothed = pl.pallas_call(
        velocity_kernel,
        out_shape=jax.ShapeDtypeStruct(new_v.shape, f32),
        in_specs=[vmem, vmem],
        out_specs=anywhere,
        scratch_shapes=[pltpu.SemaphoreType.DMA((3,))],
        cost_estimate=pl.CostEstimate(flops=20_000_000, bytes_accessed=1_600_000, transcendentals=0),
        compiler_params=pltpu.CompilerParams(vmem_limit_bytes=4 * 2**20),
        name="velocity",
    )(new_v, outs[0])

    for k in range(1, n_wide):
        late[k] = send(late[k], k)
    for k in range(2, n_wide, 2):
        pairs[k + 1] = send(pairs[k], 1)
    coarse = pl.pallas_call(
        functools.partial(collect_kernel, n_wide),
        out_shape=jax.ShapeDtypeStruct((3, CP_DEV, PV), f32),
        in_specs=[vmem] * (2 * n_wide - 1),
        out_specs=anywhere,
        scratch_shapes=[
            pltpu.VMEM((3, CP_DEV, PV), f32),
            pltpu.SemaphoreType.DMA((3 * PIECES,)),
        ],
        compiler_params=pltpu.CompilerParams(vmem_limit_bytes=8 * 2**20),
        name="collect",
    )(*late, early[0], *(pairs[k] for k in range(2, n_wide)))
    return smoothed.reshape(velocity.shape), coarse.transpose(1, 0, 2)[None]


def solution(mesh):
    in_specs = (
        P(None, "grp", "wide", None),
        P(None, "grp", "wide", None),
        P("grp", "wide", None),
        P(None, "grp", "wide", None),
        P("grp", "wide"),
        P("grp", "wide"),
    )
    out_specs = (P(None, "grp", "wide", None), P("grp", "wide", None, None))
    return jax.shard_map(
        on_device, mesh=mesh, in_specs=in_specs, out_specs=out_specs, check_vma=False
    )
```
